128 devices in a mesh: section: 2 (over core), tp: 8 (over z_lo, x), fsdp: 8 (over z_hi, y).
Axes of the slice: x: 4, y: 4, z: 4 (z_hi: 2, z_lo: 2; z = z_hi * 2 + z_lo), core: 2. Of those that a mesh axis runs over, the one named last changes fastest.
Arguments:
- normed: bfloat16 [2, 1024, 4608], P('section', 'tp', 'fsdp'), may hold values from -6 to 6
- cotangent: bfloat16 [2, 1024, 4608], P('section', 'tp', 'fsdp'), may hold values from -6 to 6
- w_gate: bfloat16 [2, 4608, 18432], P('section', 'fsdp', 'tp'), may hold values from -0.09375 to 0.09375
- w_up: bfloat16 [2, 4608, 18432], P('section', 'fsdp', 'tp'), may hold values from -0.09375 to 0.09375
- w_down: bfloat16 [2, 4608, 18432], P('section', 'fsdp', 'tp'), may hold values from -0.046875 to 0.046875
Outputs:
- passed: bfloat16 [2, 1024, 4608], P('section', 'tp', 'fsdp')
- grad_gate: bfloat16 [2, 4608, 18432], P('section', 'fsdp', 'tp')
- grad_up: bfloat16 [2, 4608, 18432], P('section', 'fsdp', 'tp')
- grad_down: bfloat16 [2, 4608, 18432], P('section', 'fsdp', 'tp')
The draws below stay inside these ranges and needn't reach their ends.
All inputs are finite; a program needn't handle non-finite values.
Results may differ from the reference program's by a relative error of at most 0.012.
Values may be sent and summed in bfloat16 or wider, within the bound.
A program may use at most 192 MiB of HBM per device.

```python
import math
import jax
import jax.numpy as jnp

D = 4608
FF = 18432
TOKENS = 1024


def block_scale(rng, shape, cuts, low, top_value):
    def one(axis_at, blocks):
        draws = jax.random.uniform(jax.random.fold_in(jax.random.fold_in(rng, 6), axis_at), (blocks,), jnp.float32, low / len(cuts), top_value / len(cuts))
        return jnp.repeat(jnp.exp(draws), shape[axis_at] // blocks).reshape((-1,) + (1,) * (len(shape) - axis_at - 1))

    level = one(*cuts[0])
    for cut in cuts[1:]:
        level = level * one(*cut)
    return level


def centred(stream_key, shape, width, limit, shards=(), dtype=jnp.bfloat16):
    drawn = width * jax.random.normal(stream_key, shape, jnp.float32)
    if shards:
        drawn = drawn * block_scale(stream_key, shape, shards, -0.22, 0.18)
    return jnp.clip(drawn, -limit, limit).astype(dtype)


def setup_inputs(seed: int = 0) -> dict:
    key_list = jax.random.split(jax.random.key(seed), 6)
    normed = centred(key_list[0], (2, TOKENS, D), 1.0, 6.0, ((0, 2), (1, 8), (2, 8)))
    cotangent = centred(key_list[1], (2, TOKENS, D), 1.0, 6.0, ((0, 2), (1, 8), (2, 8)))
    w_gate = centred(key_list[2], (2, D, FF), D ** -0.5, 0.09375, ((0, 2), (1, 8), (2, 8)))
    w_up = centred(key_list[3], (2, D, FF), D ** -0.5, 0.09375, ((0, 2), (1, 8), (2, 8)))
    w_down = centred(key_list[4], (2, D, FF), FF ** -0.5, 0.046875, ((0, 2), (1, 8), (2, 8)))
    return {"normed": normed, "cotangent": cotangent, "w_gate": w_gate, "w_up": w_up, "w_down": w_down}


def activate(gate, up, back):
    coeff = math.sqrt(2.0 / math.pi)
    inner = jnp.tanh(coeff * (gate + 0.044715 * gate * gate * gate))
    act = 0.5 * gate * (1.0 + inner)
    slope = 0.5 * (1.0 + inner) + 0.5 * gate * (1.0 - inner * inner) * coeff * (1.0 + 3.0 * 0.044715 * gate * gate)
    hidden = (act * up).astype(jnp.bfloat16)
    d_gate = (back * up * slope).astype(jnp.bfloat16)
    d_up = (back * act).astype(jnp.bfloat16)
    return (hidden, d_gate, d_up)

def layer_back(rows, cot, wgate, wup, wdown):
    gate = jnp.dot(rows, wgate, preferred_element_type=jnp.float32)
    up = jnp.dot(rows, wup, preferred_element_type=jnp.float32)
    back = jnp.dot(cot, wdown, preferred_element_type=jnp.float32)
    hidden, d_gate, d_up = activate(gate, up, back)
    scale = 1.0 / math.sqrt(TOKENS)
    g_gate = (jnp.dot(rows.T, d_gate, preferred_element_type=jnp.float32) * scale).astype(jnp.bfloat16)
    g_up = (jnp.dot(rows.T, d_up, preferred_element_type=jnp.float32) * scale).astype(jnp.bfloat16)
    g_down = (jnp.dot(cot.T, hidden, preferred_element_type=jnp.float32) * scale).astype(jnp.bfloat16)
    branch = jnp.dot(d_gate, wgate.T, preferred_element_type=jnp.float32) + jnp.dot(d_up, wup.T, preferred_element_type=jnp.float32)
    handed = (cot.astype(jnp.float32) + branch).astype(jnp.bfloat16)
    return (handed, g_gate, g_up, g_down)

def reference(normed, cotangent, w_gate, w_up, w_down):
    first = layer_back(normed[0], cotangent[0], w_gate[0], w_up[0], w_down[0])
    second = layer_back(normed[1], cotangent[1], w_gate[1], w_up[1], w_down[1])
    passed = jnp.stack([second[0], first[0]])
    grad_gate = jnp.stack([first[1], second[1]])
    grad_up = jnp.stack([first[2], second[2]])
    grad_down = jnp.stack([first[3], second[3]])
    return (passed, grad_gate, grad_up, grad_down)
```

```python
import functools
import math

import jax
import jax.numpy as jnp
from jax import lax
from jax.experimental import pallas as pl
from jax.experimental.pallas import tpu as pltpu
from jax.sharding import PartitionSpec as P

MESH = pl.DeviceIdType.MESH
CHUNK = 256
LAGS = {"B": 1, "C": 2, "D": 3, "E": 4, "H": 5}
F32 = jnp.float32
BF16 = jnp.bfloat16


def activate(gate, up, back):
    coeff = math.sqrt(2.0 / math.pi)
    inner = jnp.tanh(coeff * (gate + 0.044715 * gate * gate * gate))
    act = 0.5 * gate * (1.0 + inner)
    slope = 0.5 * (1.0 + inner) + 0.5 * gate * (1.0 - inner * inner) * coeff * (
        1.0 + 3.0 * 0.044715 * gate * gate
    )
    return act * up, back * up * slope, back * act


def kernel(
    n_hbm, c_hbm, wg_hbm, wu_hbm, wd_hbm,
    passed, gg_hbm, gu_hbm, gd_hbm,
    rows, rows_t, weights, part, arrived, grads, branch, staged, leaving, landed, other_cot,
    load_sem, weight_sem, out_sem, head_sem, head_send, recv_sem, rs_send, ag_send, tail_recv, tail_send,
    cot_sem, cot_send,
):
    chunks = weights.shape[0]
    chunk = weights.shape[2] // 3
    total = 4 * 2 * rows.shape[3]
    half = rows.shape[3] // 2
    section = lax.axis_index("section")
    tp = lax.axis_index("tp")
    fsdp = lax.axis_index("fsdp")
    zl, x = tp // 4, tp % 4
    zh, y = fsdp // 4, fsdp % 4
    oz = 1 - zh
    ol = 1 - zl
    y1, y2, y3 = (y + 1) % 4, (y + 2) % 4, (y + 3) % 4
    x1, x2, x3 = (x + 1) % 4, (x + 2) % 4, (x + 3) % 4
    to_y1, to_y2, to_y3 = ({"fsdp": zh * 4 + k} for k in (y1, y2, y3))
    to_z = {"fsdp": oz * 4 + y}
    to_x1, to_x2, to_x3 = ({"tp": zl * 4 + k} for k in (x1, x2, x3))
    to_l = {"tp": ol * 4 + x}
    others = [{"section": 1 - section, "tp": t} for t in range(8)]

    for t in range(chunks):
        for k, hbm in enumerate((wg_hbm, wu_hbm, wd_hbm)):
            pltpu.make_async_copy(
                hbm.at[0, :, t * chunk : (t + 1) * chunk],
                weights.at[t, :, k * chunk : (k + 1) * chunk],
                weight_sem.at[t],
            ).start()
    own_n = pltpu.make_async_copy(n_hbm.at[0], rows.at[0, x, zl], load_sem.at[0])
    own_c = pltpu.make_async_copy(c_hbm.at[0], rows.at[1, x, zl], load_sem.at[1])
    own_n.start()
    own_c.start()

    barrier = pltpu.get_barrier_semaphore()
    peers = [to_y1, to_y2, to_y3, to_z, to_x1, to_x2, to_x3, to_l] + others
    for peer in peers:
        pl.semaphore_signal(barrier, inc=1, device_id=peer, device_id_type=MESH)
    pl.semaphore_wait(barrier, len(peers))

    def send(src, dst, send_sem, recv, peer):
        pltpu.make_async_remote_copy(
            src_ref=src, dst_ref=dst, send_sem=send_sem, recv_sem=recv, device_id=peer, device_id_type=MESH
        ).start()

    def wait_for(ref, sem):
        pltpu.make_async_copy(ref, ref, sem).wait()

    def head(k, xx, ll, to, sem):
        send(rows.at[k, xx, ll], rows.at[k, xx, ll], head_send.at[k], head_sem.at[sem], to)

    own_n.wait()
    head(0, x, zl, to_l, 1)
    for to in (to_x1, to_x3, to_x2):
        head(0, x, zl, to, 0)
    own_c.wait()
    for to in (to_x1, to_x3, to_x2):
        head(1, x, zl, to, 2)
    head(1, x, zl, to_l, 3)
    send(rows.at[1, x, zl], other_cot, cot_send, cot_sem, {"section": 1 - section})
    wait_for(rows.at[0, 0, 0], head_sem.at[1])
    for to in (to_x1, to_x3, to_x2):
        head(0, x, ol, to, 0)
    wait_for(rows.at[1, 0:3, 0], head_sem.at[2])
    for xx in (x1, x3, x2):
        head(1, xx, zl, to_l, 3)
    wait_for(rows.at[0, 0:3], head_sem.at[0])
    wait_for(rows.at[1, 0:2], head_sem.at[3])

    branch[...] = jnp.zeros_like(branch)

    def forward(c):
        wait_for(weights.at[c], weight_sem.at[c])

        def tile(k, _):
            n_tile = rows[0, k].reshape(4 * half, rows.shape[4])
            c_tile = rows[1, k].reshape(4 * half, rows.shape[4])
            gate_up = jnp.dot(n_tile, weights[c, :, : 2 * chunk], preferred_element_type=F32)
            part[c, k, :, :, : 2 * chunk] = gate_up.astype(BF16).reshape(2, 2 * half, 2 * chunk)
            back = jnp.dot(c_tile, weights[c, :, 2 * chunk :], preferred_element_type=F32)
            part[c, k, :, :, 2 * chunk :] = back.astype(BF16).reshape(2, 2 * half, chunk)
            return 0

        lax.fori_loop(0, 4, tile, 0)

    def add(dst, src):
        dst[...] = (dst[...].astype(F32) + src[...].astype(F32)).astype(BF16)

    def rs(src, dst, c, k, to):
        send(src, dst, rs_send.at[c], recv_sem.at[c, k], to)

    def ag(c, yy, zz, k, to):
        send(grads.at[c, yy, zz], grads.at[c, yy, zz], ag_send.at[c], recv_sem.at[c, k], to)

    def start_y(c):
        rs(part.at[c, y2, 0], arrived.at[c, 0], c, 0, to_y1)
        rs(part.at[c, y2, 1], arrived.at[c, 1], c, 0, to_y3)

    def start_z(c):
        for yy in (y2, y1, y3, y):
            rs(part.at[c, yy, oz], arrived.at[c, yy], c, 0, to_z)

    def second_y(c):
        wait_for(arrived.at[c, 0:2], recv_sem.at[c, 0])
        add(part.at[c, y1, 0], arrived.at[c, 0])
        rs(part.at[c, y1], arrived.at[c, 2:4], c, 1, to_y1)
        add(part.at[c, y3, 1], arrived.at[c, 1])
        rs(part.at[c, y3], arrived.at[c, 4:6], c, 1, to_y3)

    def second_z(c):
        wait_for(arrived.at[c, 0:4], recv_sem.at[c, 0])
        add(part.at[c, y2, zh], arrived.at[c, y2])
        rs(part.at[c, y2, zh, :half], arrived.at[c, 4, :half], c, 1, to_y1)
        rs(part.at[c, y2, zh, half:], arrived.at[c, 4, half:], c, 1, to_y3)
        add(part.at[c, y1, zh], arrived.at[c, y1])
        add(part.at[c, y3, zh], arrived.at[c, y3])

    def third_y(c):
        wait_for(arrived.at[c, 2:6], recv_sem.at[c, 1])
        part[c, y, oz] = (
            part[c, y, oz].astype(F32) + arrived[c, 2 + oz].astype(F32) + arrived[c, 4 + oz].astype(F32)
        ).astype(BF16)
        rs(part.at[c, y, oz], arrived.at[c, 6], c, 2, to_z)

    def third_z(c):
        wait_for(arrived.at[c, 4], recv_sem.at[c, 1])
        add(part.at[c, y1, zh, :half], arrived.at[c, 4, :half])
        rs(part.at[c, y1, zh], arrived.at[c, 5], c, 2, to_y1)
        add(part.at[c, y3, zh, half:], arrived.at[c, 4, half:])
        rs(part.at[c, y3, zh], arrived.at[c, 6], c, 2, to_y3)

    def finish(c, terms):
        summed = part[c, y, zh].astype(F32)
        for t in terms:
            summed = summed + arrived[c, t].astype(F32)
        hidden, d_gate, d_up = activate(summed[:, :chunk], summed[:, chunk : 2 * chunk], summed[:, 2 * chunk :])
        grads[c, y, zh, :, :chunk] = d_gate.astype(BF16)
        grads[c, y, zh, :, chunk : 2 * chunk] = d_up.astype(BF16)
        grads[c, y, zh, :, 2 * chunk :] = hidden.astype(BF16)

    def finish_y(c):
        wait_for(arrived.at[c, 6], recv_sem.at[c, 2])
        finish(c, (2 + zh, 4 + zh, 6))
        ag(c, y, zh, 3, to_z)
        for to in (to_y1, to_y3, to_y2):
            ag(c, y, zh, 4, to)

    def finish_z(c):
        wait_for(arrived.at[c, 5:7], recv_sem.at[c, 2])
        finish(c, (y, 5, 6))
        for to in (to_y1, to_y3, to_y2):
            ag(c, y, zh, 3, to)
        ag(c, y, zh, 4, to_z)

    def spread_y(c):
        wait_for(grads.at[c, 0, 0], recv_sem.at[c, 3])
        for to in (to_y1, to_y3, to_y2):
            ag(c, y, oz, 4, to)

    def spread_z(c):
        wait_for(grads.at[c, 0:3, 0], recv_sem.at[c, 3])
        for yy in (y1, y3, y2):
            ag(c, yy, zh, 4, to_z)

    def take_y(c):
        wait_for(grads.at[c, 0:3], recv_sem.at[c, 4])

    def take_z(c):
        wait_for(grads.at[c, 0:2], recv_sem.at[c, 4])

    def to_branch(c):
        def tile(k, _):
            g_tile = grads[c, k, :, :, : 2 * chunk].reshape(4 * half, 2 * chunk)
            back = lax.dot_general(
                g_tile, weights[c, :, : 2 * chunk], (((1,), (1,)), ((), ())), preferred_element_type=F32
            )
            branch[k] += back.reshape(2, 2 * half, back.shape[1])
            return 0

        lax.fori_loop(0, 4, tile, 0)

    def transposes():
        for k in range(2):
            for r in range(8):
                rows_t[k, :, r * 2 * half : (r + 1) * 2 * half] = rows[k, r // 2, r % 2].T

    outs = (gg_hbm, gu_hbm, gd_hbm)

    def weight_grads(c):
        slot = lax.rem(c, 2)

        @pl.when(c >= 2)
        def _():
            wait_for(staged.at[slot], out_sem.at[slot])

        m = rows_t.shape[1] // 3
        scale = 1.0 / math.sqrt(total)

        def tile(k, _):
            at = pl.ds(pl.multiple_of(k * m, m), m)
            d_in = grads[c, :, :, :, : 2 * chunk].reshape(total, 2 * chunk)
            a = jnp.dot(rows_t[0, at, :], d_in, preferred_element_type=F32) * scale
            staged[slot, at, : 2 * chunk] = a.astype(BF16)
            hid = grads[c, :, :, :, 2 * chunk :].reshape(total, chunk)
            b = jnp.dot(rows_t[1, at, :], hid, preferred_element_type=F32) * scale
            staged[slot, at, 2 * chunk :] = b.astype(BF16)
            return 0

        lax.fori_loop(0, 3, tile, 0)
        at = pl.ds(pl.multiple_of(c * chunk, chunk), chunk)
        for k, hbm in enumerate(outs):
            pltpu.make_async_copy(
                staged.at[slot, :, k * chunk : (k + 1) * chunk], hbm.at[0, :, at], out_sem.at[slot]
            ).start()

    def both(c, for_y, for_z):
        @pl.when((c >= 0) & (c < chunks) & (lax.rem(c, 2) == 0))
        def _():
            for_y(c)

        @pl.when((c >= 0) & (c < chunks) & (lax.rem(c, 2) == 1))
        def _():
            for_z(c)

    def step(i, _):
        @pl.when(i < chunks)
        def _():
            forward(i)

        both(i, start_y, start_z)
        both(i - LAGS["B"], second_y, second_z)
        both(i - LAGS["C"], third_y, third_z)
        both(i - LAGS["D"], finish_y, finish_z)
        both(i - LAGS["E"], spread_y, spread_z)

        @pl.when(i == 2)
        def _():
            transposes()

        c = i - LAGS["H"]
        both(c, take_y, take_z)

        @pl.when(c >= 0)
        def _():
            to_branch(c)

        @pl.when(c == chunks - 1)
        def _():
            for r in range(8):
                leaving[r] = branch[r // 2, r % 2].astype(BF16)
            for r in range(8):
                t = (r % 2) * 4 + r // 2
                send(leaving.at[r], landed.at[tp], tail_send, tail_recv, others[t])

        @pl.when(c >= 0)
        def _():
            weight_grads(c)

        return 0

    lax.fori_loop(0, chunks + LAGS["H"], step, 0)

    wait_for(other_cot, cot_sem)
    wait_for(landed, tail_recv)
    summed = landed[0].astype(F32)
    for r in range(1, 8):
        summed = summed + landed[r].astype(F32)
    passed[0] = (other_cot[...].astype(F32) + summed).astype(BF16)

    def drain(c, _):
        wait_for(arrived.at[c], rs_send.at[c])
        wait_for(arrived.at[c], ag_send.at[c])
        return 0

    lax.fori_loop(0, chunks, drain, 0)
    for k in range(2):
        wait_for(landed.at[0:7], head_send.at[k])
    wait_for(other_cot, cot_send)
    wait_for(leaving, tail_send)
    for slot in range(2):
        wait_for(staged.at[slot], out_sem.at[slot])


def local(normed, cotangent, w_gate, w_up, w_down):
    _, length, depth = normed.shape
    width = w_gate.shape[2]
    chunks = width // CHUNK
    wide = 3 * CHUNK
    anywhere = pl.BlockSpec(memory_space=pl.ANY)
    dma = pltpu.SemaphoreType.DMA
    return pl.pallas_call(
        kernel,
        out_shape=(
            jax.ShapeDtypeStruct(normed.shape, BF16),
            jax.ShapeDtypeStruct(w_gate.shape, BF16),
            jax.ShapeDtypeStruct(w_gate.shape, BF16),
            jax.ShapeDtypeStruct(w_gate.shape, BF16),
        ),
        in_specs=[anywhere] * 5,
        out_specs=(pl.BlockSpec(memory_space=pltpu.VMEM), anywhere, anywhere, anywhere),
        scratch_shapes=[
            pltpu.VMEM((2, 4, 2, length, depth), BF16),
            pltpu.VMEM((2, depth, 8 * length), BF16),
            pltpu.VMEM((chunks, depth, wide), BF16),
            pltpu.VMEM((chunks, 4, 2, length, wide), BF16),
            pltpu.VMEM((chunks, 7, length, wide), BF16),
            pltpu.VMEM((chunks, 4, 2, length, wide), BF16),
            pltpu.VMEM((4, 2, length, depth), F32),
            pltpu.VMEM((2, depth, wide), BF16),
            pltpu.VMEM((8, length, depth), BF16),
            pltpu.VMEM((8, length, depth), BF16),
            pltpu.VMEM((length, depth), BF16),
            dma((2,)),
            dma((chunks,)),
            dma((2,)),
            dma((4,)),
            dma((2,)),
            dma((chunks, 5)),
            dma((chunks,)),
            dma((chunks,)),
            dma(()),
            dma(()),
            dma(()),
            dma(()),
        ],
        compiler_params=pltpu.CompilerParams(
            collective_id=0, has_side_effects=True, vmem_limit_bytes=67_043_328
        ),
        name="geglu_relay",
    )(normed, cotangent, w_gate, w_up, w_down)


def solution(mesh):
    in_specs = (
        P("section", "tp", "fsdp"),
        P("section", "tp", "fsdp"),
        P("section", "fsdp", "tp"),
        P("section", "fsdp", "tp"),
        P("section", "fsdp", "tp"),
    )
    out_specs = (
        P("section", "tp", "fsdp"),
        P("section", "fsdp", "tp"),
        P("section", "fsdp", "tp"),
        P("section", "fsdp", "tp"),
    )
    return jax.shard_map(local, mesh=mesh, in_specs=in_specs, out_specs=out_specs, check_vma=False)
```

```python
import functools
import math

import jax
import jax.numpy as jnp
from jax import lax
from jax.experimental import pallas as pl
from jax.experimental.pallas import tpu as pltpu
from jax.sharding import PartitionSpec as P

MESH = pl.DeviceIdType.MESH
CHUNK = 256
LAG_SUM = ({"y": (0, 2, 3), "z": (0, 2, 3)}, {"y": (3, 4, 6), "z": (3, 4, 6)})
LAG_OUT = ({"y": (7, 8, 9, 10), "z": (7, 8, 9, 10)}, {"y": (13, 14, 15, 16), "z": (13, 14, 15, 17)})
LAST = 17
F32 = jnp.float32
BF16 = jnp.bfloat16


def activate(gate, up, back):
    coeff = math.sqrt(2.0 / math.pi)
    inner = jnp.tanh(coeff * (gate + 0.044715 * gate * gate * gate))
    act = 0.5 * gate * (1.0 + inner)
    slope = 0.5 * (1.0 + inner) + 0.5 * gate * (1.0 - inner * inner) * coeff * (
        1.0 + 3.0 * 0.044715 * gate * gate
    )
    return act * up, back * up * slope, back * act


def sums_z(c):
    return (c > 0) & (lax.rem(c, 2) == 0)


def spreads_z(c):
    return lax.rem(c, 2) == 1


def kernel(
    n_hbm, c_hbm, wg_hbm, wu_hbm, wd_hbm,
    passed, gg_hbm, gu_hbm, gd_hbm,
    own, rows, rows_t, weights, part0, part1, arrived0, arrived1, grads0, grads1, branch,
    staged0, staged1, leaving, landed, other_cot,
    load_sem, weight_sem, out_sem, head_sem, head_send, recv_sem, send_sem, tail_recv, tail_send, cot_sem, cot_send,
):
    parts, arriveds, gradss, stageds = (part0, part1), (arrived0, arrived1), (grads0, grads1), (staged0, staged1)
    chunks = weights.shape[0]
    chunk = weights.shape[2] // 3
    depth = rows.shape[4]
    length = rows.shape[3]
    half = length // 2
    total = 8 * length
    low, high = pl.ds(0, half), pl.ds(half, half)
    columns = (pl.ds(0, 2 * chunk), pl.ds(2 * chunk, chunk))
    section = lax.axis_index("section")
    tp = lax.axis_index("tp")
    fsdp = lax.axis_index("fsdp")
    zl, x = tp // 4, tp % 4
    zh, y = fsdp // 4, fsdp % 4
    oz = 1 - zh
    ol = 1 - zl
    y1, y2, y3 = (y + 1) % 4, (y + 2) % 4, (y + 3) % 4
    x1, x2, x3 = (x + 1) % 4, (x + 2) % 4, (x + 3) % 4
    to_y1, to_y3 = ({"fsdp": zh * 4 + k} for k in (y1, y3))
    to_z = {"fsdp": oz * 4 + y}
    to_x1, to_x2, to_x3 = ({"tp": zl * 4 + k} for k in (x1, x2, x3))
    to_l = {"tp": ol * 4 + x}
    others = [{"section": 1 - section, "tp": t} for t in range(8)]

    loads = [pltpu.make_async_copy(hbm.at[0], own.at[k], load_sem.at[k]) for k, hbm in enumerate((n_hbm, c_hbm))]
    for load in loads:
        load.start()

    barrier = pltpu.get_barrier_semaphore()
    peers = [to_y1, to_y3, to_z, to_x1, to_x2, to_x3, to_l] + others
    for peer in peers:
        pl.semaphore_signal(barrier, inc=1, device_id=peer, device_id_type=MESH)

    for t in range(chunks):
        for k, hbm in enumerate((wg_hbm, wu_hbm, wd_hbm)):
            pltpu.make_async_copy(
                hbm.at[0, :, t * chunk : (t + 1) * chunk],
                weights.at[t, :, k * chunk : (k + 1) * chunk],
                weight_sem.at[t, k // 2],
            ).start()

    for k, load in enumerate(loads):
        load.wait()
        rows[k, x, zl] = own[k].T

    def send(src, dst, sender, recv, peer):
        pltpu.make_async_remote_copy(
            src_ref=src, dst_ref=dst, send_sem=sender, recv_sem=recv, device_id=peer, device_id_type=MESH
        ).start()

    def wait_for(ref, sem):
        pltpu.make_async_copy(ref, ref, sem).wait()

    def head(k, xx, ll, which, sem, *peers):
        ref = rows.at[k, xx, ll, which]
        for peer in peers:
            send(ref, ref, head_send.at[k], head_sem.at[k, sem], peer)

    def head_start(k):
        head(k, x, zl, high, 2, to_x1, to_x3, to_x2)
        head(k, x, zl, low, 0, to_l)
        head(k, x, zl, high, 3, to_l)
        head(k, x, zl, low, 1, to_x1, to_x3, to_x2)

    def head_middle(k):
        wait_for(rows.at[k, 0, 0, low], head_sem.at[k, 0])
        head(k, x, ol, low, 1, to_x1, to_x3, to_x2)
        wait_for(rows.at[k, 0:3, 0, low], head_sem.at[k, 2])
        for xx in (x1, x3, x2):
            head(k, xx, zl, high, 3, to_l)

    def head_end(k):
        wait_for(rows.at[k, 0:3, 0], head_sem.at[k, 1])
        wait_for(rows.at[k, 0:2, 0], head_sem.at[k, 3])

    pl.semaphore_wait(barrier, len(peers))
    head_start(0)
    head_start(1)
    send(rows.at[1, x, zl], other_cot, cot_send, cot_sem, {"section": 1 - section})
    branch[...] = jnp.zeros_like(branch)
    head_middle(0)
    head_end(0)

    def forward(s, c):
        wait_for(weights.at[c, :, columns[s]], weight_sem.at[c, s])

        def tile(k, _):
            left = rows[s, k].reshape(2 * length, depth)
            out = jnp.dot(left, weights[c, :, columns[s]], preferred_element_type=F32)
            parts[s][c, k] = out.astype(BF16).reshape(2, length, out.shape[1])
            return 0

        lax.fori_loop(0, 4, tile, 0)

    def add(dst, src):
        dst[...] = (dst[...].astype(F32) + src[...].astype(F32)).astype(BF16)

    def move(src, dst, s, c, k, *peers):
        for peer in peers:
            send(src, dst, send_sem.at[k // 3, s, c], recv_sem.at[s, c, k], peer)

    def sum_y(s, stage, c):
        part, arrived = parts[s].at[c], arriveds[s].at[c]
        if stage == 0:
            forward(s, c)
            move(part.at[y2, 0], arrived.at[0], s, c, 0, to_y1)
            move(part.at[y2, 1], arrived.at[1], s, c, 0, to_y3)
        elif stage == 1:
            wait_for(arrived.at[0:2], recv_sem.at[s, c, 0])
            add(part.at[y1, 0], arrived.at[0])
            move(part.at[y1], arrived.at[2:4], s, c, 1, to_y1)
            add(part.at[y3, 1], arrived.at[1])
            move(part.at[y3], arrived.at[4:6], s, c, 1, to_y3)
        else:
            wait_for(arrived.at[2:6], recv_sem.at[s, c, 1])
            part[y, oz] = (
                part[y, oz].astype(F32) + arrived[2 + oz].astype(F32) + arrived[4 + oz].astype(F32)
            ).astype(BF16)
            move(part.at[y, oz], arrived.at[6], s, c, 2, to_z)

    def sum_z(s, stage, c):
        part, arrived = parts[s].at[c], arriveds[s].at[c]
        if stage == 0:
            forward(s, c)
            for yy in (y2, y1, y3, y):
                move(part.at[yy, oz], arrived.at[yy], s, c, 0, to_z)
        elif stage == 1:
            wait_for(arrived.at[0:4], recv_sem.at[s, c, 0])
            add(part.at[y2, zh], arrived.at[y2])
            move(part.at[y2, zh, low], arrived.at[4, low], s, c, 1, to_y1)
            move(part.at[y2, zh, high], arrived.at[4, high], s, c, 1, to_y3)
            add(part.at[y1, zh], arrived.at[y1])
            add(part.at[y3, zh], arrived.at[y3])
        else:
            wait_for(arrived.at[4], recv_sem.at[s, c, 1])
            add(part.at[y1, zh, low], arrived.at[4, low])
            move(part.at[y1, zh], arrived.at[5], s, c, 2, to_y1)
            add(part.at[y3, zh, high], arrived.at[4, high])
            move(part.at[y3, zh], arrived.at[6], s, c, 2, to_y3)

    def final_y(s, c):
        wait_for(arriveds[s].at[c, 6], recv_sem.at[s, c, 2])
        return final(s, c, (2 + zh, 4 + zh, 6))

    def final_z(s, c):
        wait_for(arriveds[s].at[c, 5:7], recv_sem.at[s, c, 2])
        return final(s, c, (y, 5, 6))

    def final(s, c, terms):
        out = parts[s][c, y, zh].astype(F32)
        for t in terms:
            out = out + arriveds[s][c, t].astype(F32)
        return out

    def finish(c, done):
        gate_up, back = done(0, c), done(1, c)
        hidden, d_gate, d_up = activate(gate_up[:, :chunk], gate_up[:, chunk:], back)
        grads0[c, y, zh, :, :chunk] = d_gate.astype(BF16)
        grads0[c, y, zh, :, chunk:] = d_up.astype(BF16)
        grads1[c, y, zh] = hidden.astype(BF16)

    def spread(s, c, yy, zz, k, *peers, which=None):
        ref = gradss[s].at[c, yy, zz] if which is None else gradss[s].at[c, yy, zz, which]
        move(ref, ref, s, c, 3 + k, *peers)

    def spread_y(s, stage, c):
        grads = gradss[s].at[c]
        if stage == 0:
            spread(s, c, y, zh, 0, to_z)
            spread(s, c, y, zh, 1, to_y1, to_y3)
        elif stage == 1:
            wait_for(grads.at[0, 0], recv_sem.at[s, c, 3])
            spread(s, c, y, oz, 1, to_y1, to_y3)
        elif stage == 2:
            wait_for(grads.at[0:2], recv_sem.at[s, c, 4])
            spread(s, c, y3, 0, 2, to_y1)
            spread(s, c, y1, 1, 2, to_y3)
        else:
            wait_for(grads.at[0], recv_sem.at[s, c, 5])
            use(s, c)

    def spread_z(s, stage, c):
        grads = gradss[s].at[c]
        if stage == 0:
            spread(s, c, y, zh, 0, to_y1, to_y3)
            spread(s, c, y, zh, 2, to_z)
        elif stage == 1:
            wait_for(grads.at[0], recv_sem.at[s, c, 3])
            spread(s, c, y3, zh, 1, to_y1, which=low)
            spread(s, c, y1, zh, 1, to_y3, which=high)
            spread(s, c, y1, zh, 2, to_z)
            spread(s, c, y3, zh, 2, to_z)
        elif stage == 2:
            wait_for(grads.at[0, 0], recv_sem.at[s, c, 4])
            spread(s, c, y2, zh, 2, to_z)
        else:
            wait_for(grads.at[0:2], recv_sem.at[s, c, 5])
            use(s, c)

    def to_branch(c):
        def tile(k, _):
            back = lax.dot_general(
                grads0[c, k].reshape(2 * length, 2 * chunk),
                weights[c, :, columns[0]],
                (((1,), (1,)), ((), ())),
                preferred_element_type=F32,
            )
            branch[k] += back.reshape(2, length, depth)
            return 0

        lax.fori_loop(0, 4, tile, 0)

    def leave():
        for r in range(8):
            leaving[r] = branch[r // 2, r % 2].astype(BF16)
        for r in range(8):
            t = (r % 2) * 4 + r // 2
            send(leaving.at[r], landed.at[tp], tail_send, tail_recv, others[t])

    def use(s, c):
        if s == 0:
            to_branch(c)
            pl.when(c == chunks - 1)(leave)
        slot = lax.rem(c, 2)
        staged = stageds[s]

        @pl.when(c >= 2)
        def _():
            wait_for(staged.at[slot], out_sem.at[s, slot])

        m = depth // 3
        scale = 1.0 / math.sqrt(total)

        def tile(k, _):
            at = pl.ds(pl.multiple_of(k * m, m), m)
            right = gradss[s][c].reshape(total, staged.shape[2])
            out = jnp.dot(rows_t[s, at, :], right, preferred_element_type=F32) * scale
            staged[slot, at, :] = out.astype(BF16)
            return 0

        lax.fori_loop(0, 3, tile, 0)
        at = pl.ds(pl.multiple_of(c * chunk, chunk), chunk)
        for k, hbm in enumerate(((gg_hbm, gu_hbm), (gd_hbm,))[s]):
            pltpu.make_async_copy(
                staged.at[slot, :, k * chunk : (k + 1) * chunk], hbm.at[0, :, at], out_sem.at[s, slot]
            ).start()

    def transposes():
        for k in range(2):
            for r in range(8):
                rows_t[k, :, r * length : (r + 1) * length] = rows[k, r // 2, r % 2].T

    def at_step(i, lags, stage, kind, for_y, for_z):
        for name, what in (("z", for_z), ("y", for_y)):
            c = i - lags[name][stage]
            picked = kind(c) if name == "z" else jnp.logical_not(kind(c))

            @pl.when((c >= 0) & (c < chunks) & picked)
            def _():
                what(c)

    def step(i, _):
        @pl.when(i == 1)
        def _():
            head_middle(1)

        @pl.when(i == LAG_SUM[1]["y"][0])
        def _():
            head_end(1)

        for stage in range(3):
            for s in range(2):
                at_step(
                    i, LAG_SUM[s], stage, sums_z,
                    functools.partial(sum_y, s, stage), functools.partial(sum_z, s, stage),
                )
        c = i - LAG_OUT[0]["y"][0]
        for pick, done in ((sums_z(c), final_z), (jnp.logical_not(sums_z(c)), final_y)):

            @pl.when((c >= 0) & (c < chunks) & pick)
            def _():
                finish(c, done)

        for stage in range(4):
            for s in range(2):
                at_step(
                    i, LAG_OUT[s], stage, spreads_z,
                    functools.partial(spread_y, s, stage), functools.partial(spread_z, s, stage),
                )
        pl.when(i == LAG_SUM[1]["y"][0] + 1)(transposes)
        return 0

    lax.fori_loop(0, chunks + LAST, step, 0)

    wait_for(other_cot, cot_sem)
    wait_for(landed, tail_recv)
    summed = landed[0].astype(F32)
    for r in range(1, 8):
        summed = summed + landed[r].astype(F32)
    passed[0] = (other_cot[...].astype(F32) + summed).astype(BF16).T

    def drain(c, _):
        for k in range(2):
            for s in range(2):
                wait_for(arriveds[s].at[c], send_sem.at[k, s, c])
        return 0

    lax.fori_loop(0, chunks, drain, 0)
    for k in range(2):
        wait_for(landed.at[0:7], head_send.at[k])
    wait_for(other_cot, cot_send)
    wait_for(leaving, tail_send)
    for s in range(2):
        for slot in range(2):
            wait_for(stageds[s].at[slot], out_sem.at[s, slot])


def local(normed, cotangent, w_gate, w_up, w_down):
    _, length, depth = normed.shape
    width = w_gate.shape[2]
    chunks = width // CHUNK
    wide = (2 * CHUNK, CHUNK)
    anywhere = pl.BlockSpec(memory_space=pl.ANY)
    dma = pltpu.SemaphoreType.DMA
    flipped = jax.ShapeDtypeStruct((1, depth, length), BF16)
    passed, *grads = pl.pallas_call(
        kernel,
        out_shape=(flipped, *[jax.ShapeDtypeStruct(w_gate.shape, BF16)] * 3),
        in_specs=[anywhere] * 5,
        out_specs=(pl.BlockSpec(memory_space=pltpu.VMEM), anywhere, anywhere, anywhere),
        scratch_shapes=[
            pltpu.VMEM((2, depth, length), BF16),
            pltpu.VMEM((2, 4, 2, length, depth), BF16),
            pltpu.VMEM((2, depth, 8 * length), BF16),
            pltpu.VMEM((chunks, depth, 3 * CHUNK), BF16),
            *[pltpu.VMEM((chunks, 4, 2, length, w), BF16) for w in wide],
            *[pltpu.VMEM((chunks, 7, length, w), BF16) for w in wide],
            *[pltpu.VMEM((chunks, 4, 2, length, w), BF16) for w in wide],
            pltpu.VMEM((4, 2, length, depth), F32),
            *[pltpu.VMEM((2, depth, w), BF16) for w in wide],
            pltpu.VMEM((8, length, depth), BF16),
            pltpu.VMEM((8, length, depth), BF16),
            pltpu.VMEM((length, depth), BF16),
            dma((2,)),
            dma((chunks, 2)),
            dma((2, 2)),
            dma((2, 4)),
            dma((2,)),
            dma((2, chunks, 6)),
            dma((2, 2, chunks)),
            dma(()),
            dma(()),
            dma(()),
            dma(()),
        ],
        compiler_params=pltpu.CompilerParams(
            collective_id=0, has_side_effects=True, vmem_limit_bytes=67_043_328
        ),
        name="geglu_relay",
    )(jnp.swapaxes(normed, 1, 2), jnp.swapaxes(cotangent, 1, 2), w_gate, w_up, w_down)
    return (jnp.swapaxes(passed, 1, 2), *grads)


def solution(mesh):
    in_specs = (
        P("section", "tp", "fsdp"),
        P("section", "tp", "fsdp"),
        P("section", "fsdp", "tp"),
        P("section", "fsdp", "tp"),
        P("section", "fsdp", "tp"),
    )
    out_specs = (
        P("section", "tp", "fsdp"),
        P("section", "fsdp", "tp"),
        P("section", "fsdp", "tp"),
        P("section", "fsdp", "tp"),
    )
    return jax.shard_map(local, mesh=mesh, in_specs=in_specs, out_specs=out_specs, check_vma=False)
```

```python
import functools
import math

import jax
import jax.numpy as jnp
from jax import lax
from jax.experimental import pallas as pl
from jax.experimental.pallas import tpu as pltpu
from jax.sharding import PartitionSpec as P

MESH = pl.DeviceIdType.MESH
CHUNK = 256
SUMS_Z = (2, 4, 5, 6)
SPREADS_Z = (0, 1, 7)
LAGS = {
    (0, 0): (0, 0),
    (0, 1): (20, 4),
    (0, 2): (27, 22),
    (0, 3): (46, 46),
    (0, 4): (81, 79),
    (0, 5): (84, 84),
    (0, 6): (90, 89),
    (1, 0): (6, 6),
    (1, 1): (28, 12),
    (1, 2): (40, 27),
    (1, 3): (84, 87),
    (1, 4): (90, 93),
    (1, 5): (96, 99),
    (1, 6): (105, 105),
}
ORDER = (
    (1, 1),
    (1, 6),
    (1, 5),
    (1, 0),
    (1, 2),
    (1, 3),
    (1, 4),
    (0, 0),
    (0, 3),
    (0, 1),
    (0, 2),
    (0, 6),
    (0, 4),
    (0, 5),
)
HEAD_AT = 4
BACK_AT = 6
LAST = 105
F32 = jnp.float32
BF16 = jnp.bfloat16


def activate(gate, up, back):
    coeff = math.sqrt(2.0 / math.pi)
    inner = jnp.tanh(coeff * (gate + 0.044715 * gate * gate * gate))
    act = 0.5 * gate * (1.0 + inner)
    slope = 0.5 * (1.0 + inner) + 0.5 * gate * (1.0 - inner * inner) * coeff * (
        1.0 + 3.0 * 0.044715 * gate * gate
    )
    return act * up, back * up * slope, back * act


def among(c, members):
    return functools.reduce(jnp.logical_or, [c == m for m in members])


def kernel(
    n_hbm, c_hbm, wg_hbm, wu_hbm, wd_hbm,
    passed, grad_gate, grad_up, grad_down,
    own, rows, rows_t, weights, part0, part1, arrived0, arrived1, grads0, grads1, branch,
    landed, other_cot,
    load_sem, weight_sem, head_sem, head_send, recv_sem, send_sem, tail_recv, tail_send, cot_sem, cot_send,
):
    parts, arriveds, gradss = (part0, part1), (arrived0, arrived1), (grads0, grads1)
    chunks = weights.shape[0]
    chunk = weights.shape[2] // 3
    depth = rows.shape[4]
    length = rows.shape[3]
    half = length // 2
    total = 8 * length
    low, high = pl.ds(0, half), pl.ds(half, half)
    columns = (pl.ds(0, 2 * chunk), pl.ds(2 * chunk, chunk))
    section = lax.axis_index("section")
    tp = lax.axis_index("tp")
    fsdp = lax.axis_index("fsdp")
    zl, x = tp // 4, tp % 4
    zh, y = fsdp // 4, fsdp % 4
    oz = 1 - zh
    ol = 1 - zl
    y1, y2, y3 = (y + 1) % 4, (y + 2) % 4, (y + 3) % 4
    x1, x2, x3 = (x + 1) % 4, (x + 2) % 4, (x + 3) % 4
    to_y1, to_y3 = ({"fsdp": zh * 4 + k} for k in (y1, y3))
    to_z = {"fsdp": oz * 4 + y}
    to_x1, to_x2, to_x3 = ({"tp": zl * 4 + k} for k in (x1, x2, x3))
    to_l = {"tp": ol * 4 + x}
    others = [{"section": 1 - section, "tp": t} for t in range(8)]

    loads = [pltpu.make_async_copy(hbm.at[0], own.at[k], load_sem.at[k]) for k, hbm in enumerate((n_hbm, c_hbm))]
    for load in loads:
        load.start()

    barrier = pltpu.get_barrier_semaphore()
    peers = [to_y1, to_y3, to_z, to_x1, to_x2, to_x3, to_l] + others
    for peer in peers:
        pl.semaphore_signal(barrier, inc=1, device_id=peer, device_id_type=MESH)

    for t in range(chunks):
        for k, hbm in enumerate((wg_hbm, wu_hbm, wd_hbm)):
            pltpu.make_async_copy(
                hbm.at[0, :, t * chunk : (t + 1) * chunk],
                weights.at[t, :, k * chunk : (k + 1) * chunk],
                weight_sem.at[t, k // 2],
            ).start()

    for k, load in enumerate(loads):
        load.wait()
        rows[k, x, zl] = own[k].T

    def send(src, dst, sender, recv, peer):
        pltpu.make_async_remote_copy(
            src_ref=src, dst_ref=dst, send_sem=sender, recv_sem=recv, device_id=peer, device_id_type=MESH
        ).start()

    def wait_for(ref, sem):
        pltpu.make_async_copy(ref, ref, sem).wait()

    def head(k, xx, ll, which, sem, *peers):
        ref = rows.at[k, xx, ll, which]
        for peer in peers:
            send(ref, ref, head_send.at[k], head_sem.at[k, sem], peer)

    def head_start(k):
        head(k, x, zl, high, 2, to_x1, to_x3, to_x2)
        head(k, x, zl, low, 0, to_l)
        head(k, x, zl, high, 3, to_l)
        head(k, x, zl, low, 1, to_x1, to_x3, to_x2)

    def head_middle(k):
        wait_for(rows.at[k, 0, 0, low], head_sem.at[k, 0])
        head(k, x, ol, low, 1, to_x1, to_x3, to_x2)
        wait_for(rows.at[k, 0:3, 0, low], head_sem.at[k, 2])
        for xx in (x1, x3, x2):
            head(k, xx, zl, high, 3, to_l)

    def head_end(k):
        wait_for(rows.at[k, 0:3, 0], head_sem.at[k, 1])
        wait_for(rows.at[k, 0:2, 0], head_sem.at[k, 3])

    pl.semaphore_wait(barrier, len(peers))
    head_start(0)
    head_middle(0)
    head_start(1)
    send(rows.at[1, x, zl], other_cot, cot_send, cot_sem, {"section": 1 - section})
    branch[...] = jnp.zeros_like(branch)
    head_end(0)

    def forward(s, c):
        wait_for(weights.at[c, :, columns[s]], weight_sem.at[c, s])

        def tile(k, _):
            left = rows[s, k].reshape(2 * length, depth)
            out = jnp.dot(left, weights[c, :, columns[s]], preferred_element_type=F32)
            parts[s][c, k] = out.astype(BF16).reshape(2, length, out.shape[1])
            return 0

        lax.fori_loop(0, 4, tile, 0)

    def add(dst, src):
        dst[...] = (dst[...].astype(F32) + src[...].astype(F32)).astype(BF16)

    def move(src, dst, s, c, k, *peers):
        for peer in peers:
            send(src, dst, send_sem.at[k // 3, s, c], recv_sem.at[s, c, k], peer)

    def sum_y(s, stage, c):
        part, arrived = parts[s].at[c], arriveds[s].at[c]
        if stage == 0:
            forward(s, c)
            move(part.at[y2, 0], arrived.at[0], s, c, 0, to_y1)
            move(part.at[y2, 1], arrived.at[1], s, c, 0, to_y3)
        elif stage == 1:
            wait_for(arrived.at[0:2], recv_sem.at[s, c, 0])
            add(part.at[y1, 0], arrived.at[0])
            move(part.at[y1], arrived.at[2:4], s, c, 1, to_y1)
            add(part.at[y3, 1], arrived.at[1])
            move(part.at[y3], arrived.at[4:6], s, c, 1, to_y3)
        else:
            wait_for(arrived.at[2:6], recv_sem.at[s, c, 1])
            part[y, oz] = (
                part[y, oz].astype(F32) + arrived[2 + oz].astype(F32) + arrived[4 + oz].astype(F32)
            ).astype(BF16)
            move(part.at[y, oz], arrived.at[6], s, c, 2, to_z)

    def sum_z(s, stage, c):
        part, arrived = parts[s].at[c], arriveds[s].at[c]
        if stage == 0:
            forward(s, c)
            for yy in (y2, y1, y3, y):
                move(part.at[yy, oz], arrived.at[yy], s, c, 0, to_z)
        elif stage == 1:
            wait_for(arrived.at[0:4], recv_sem.at[s, c, 0])
            add(part.at[y2, zh], arrived.at[y2])
            move(part.at[y2, zh, low], arrived.at[4, low], s, c, 1, to_y1)
            move(part.at[y2, zh, high], arrived.at[4, high], s, c, 1, to_y3)
            add(part.at[y1, zh], arrived.at[y1])
            add(part.at[y3, zh], arrived.at[y3])
        else:
            wait_for(arrived.at[4], recv_sem.at[s, c, 1])
            add(part.at[y1, zh, low], arrived.at[4, low])
            move(part.at[y1, zh], arrived.at[5], s, c, 2, to_y1)
            add(part.at[y3, zh, high], arrived.at[4, high])
            move(part.at[y3, zh], arrived.at[6], s, c, 2, to_y3)

    def final_y(s, c):
        wait_for(arriveds[s].at[c, 6], recv_sem.at[s, c, 2])
        return final(s, c, (2 + zh, 4 + zh, 6))

    def final_z(s, c):
        wait_for(arriveds[s].at[c, 5:7], recv_sem.at[s, c, 2])
        return final(s, c, (y, 5, 6))

    def final(s, c, terms):
        out = parts[s][c, y, zh].astype(F32)
        for t in terms:
            out = out + arriveds[s][c, t].astype(F32)
        return out

    def finish(c, done):
        gate_up, back = done(0, c), done(1, c)
        hidden, d_gate, d_up = activate(gate_up[:, :chunk], gate_up[:, chunk:], back)
        grads0[c, y, zh, :, :chunk] = d_gate.astype(BF16)
        grads0[c, y, zh, :, chunk:] = d_up.astype(BF16)
        grads1[c, y, zh] = hidden.astype(BF16)

    def spread(s, c, yy, zz, k, *peers, which=None):
        ref = gradss[s].at[c, yy, zz] if which is None else gradss[s].at[c, yy, zz, which]
        move(ref, ref, s, c, 3 + k, *peers)

    def spread_y(s, stage, c):
        grads = gradss[s].at[c]
        if stage == 0:
            spread(s, c, y, zh, 0, to_z)
            spread(s, c, y, zh, 1, to_y1, to_y3)
        elif stage == 1:
            wait_for(grads.at[0, 0], recv_sem.at[s, c, 3])
            spread(s, c, y, oz, 1, to_y1, to_y3)
        elif stage == 2:
            wait_for(grads.at[0:2], recv_sem.at[s, c, 4])
            spread(s, c, y3, 0, 2, to_y1)
            spread(s, c, y1, 1, 2, to_y3)
        else:
            wait_for(grads.at[0], recv_sem.at[s, c, 5])
            use(s, c)

    def spread_z(s, stage, c):
        grads = gradss[s].at[c]
        if stage == 0:
            spread(s, c, y, zh, 0, to_y1, to_y3)
            spread(s, c, y, zh, 2, to_z)
        elif stage == 1:
            wait_for(grads.at[0], recv_sem.at[s, c, 3])
            spread(s, c, y3, zh, 1, to_y1, which=low)
            spread(s, c, y1, zh, 1, to_y3, which=high)
            spread(s, c, y1, zh, 2, to_z)
            spread(s, c, y3, zh, 2, to_z)
        elif stage == 2:
            wait_for(grads.at[0, 0], recv_sem.at[s, c, 4])
            spread(s, c, y2, zh, 2, to_z)
        else:
            wait_for(grads.at[0:2], recv_sem.at[s, c, 5])
            use(s, c)

    def to_branch(c):
        def tile(k, _):
            back = lax.dot_general(
                grads0[c, k].reshape(2 * length, 2 * chunk),
                weights[c, :, columns[0]],
                (((1,), (1,)), ((), ())),
                preferred_element_type=F32,
            )
            branch[k] += back.reshape(2, length, depth)
            return 0

        lax.fori_loop(0, 4, tile, 0)

    def leave():
        for k in range(2):
            wait_for(landed.at[0:7], head_send.at[k])
        for r in range(8):
            rows[0, r // 2, r % 2] = branch[r // 2, r % 2].astype(BF16)
        for r in range(8):
            t = (r % 2) * 4 + r // 2
            send(rows.at[0, r // 2, r % 2], landed.at[tp], tail_send, tail_recv, others[t])

    def use(s, c):
        if s == 0:
            to_branch(c)
            pl.when(c == chunks - 1)(leave)
        m = depth // 3
        scale = 1.0 / math.sqrt(total)

        def tile(k, _):
            at = pl.ds(pl.multiple_of(k * m, m), m)
            right = gradss[s][c].reshape(total, gradss[s].shape[4])
            out = (jnp.dot(rows_t[s, at, :], right, preferred_element_type=F32) * scale).astype(BF16)
            for q, ref in enumerate(((grad_gate, grad_up), (grad_down,))[s]):
                ref[0, at, pl.ds(pl.multiple_of(c * chunk, chunk), chunk)] = out[:, q * chunk : (q + 1) * chunk]
            return 0

        lax.fori_loop(0, 3, tile, 0)

    def transposes():
        for k in range(2):
            for r in range(8):
                rows_t[k, :, r * length : (r + 1) * length] = rows[k, r // 2, r % 2].T

    def at_step(i, lags, members, for_y, for_z):
        for lag, what, z in zip(lags, (for_z, for_y), (True, False)):
            c = i - lag
            picked = among(c, members) if z else jnp.logical_not(among(c, members))

            @pl.when((c >= 0) & (c < chunks) & picked)
            def _():
                what(c)

    def step(i, _):
        pl.when(i == HEAD_AT)(functools.partial(head_middle, 1))

        @pl.when(i == BACK_AT)
        def _():
            head_end(1)

        for s, stage in ORDER:
            if stage < 3:
                bind = functools.partial
                at_step(i, LAGS[s, stage], SUMS_Z, bind(sum_y, s, stage), bind(sum_z, s, stage))
            else:
                if (s, stage) == (0, 3):
                    at_step(
                        i, LAGS[s, stage], SUMS_Z,
                        functools.partial(finish, done=final_y), functools.partial(finish, done=final_z),
                    )
                at_step(
                    i, LAGS[s, stage], SPREADS_Z,
                    functools.partial(spread_y, s, stage - 3), functools.partial(spread_z, s, stage - 3),
                )
        pl.when(i == BACK_AT + 1)(transposes)
        return 0

    lax.fori_loop(0, chunks + LAST, step, 0)

    wait_for(other_cot, cot_sem)
    wait_for(landed, tail_recv)
    summed = landed[0].astype(F32)
    for r in range(1, 8):
        summed = summed + landed[r].astype(F32)
    passed[0] = (other_cot[...].astype(F32) + summed).astype(BF16).T

    def drain(c, _):
        for k in range(2):
            for s in range(2):
                wait_for(arriveds[s].at[c], send_sem.at[k, s, c])
        return 0

    lax.fori_loop(0, chunks, drain, 0)
    wait_for(other_cot, cot_send)
    wait_for(rows.at[0], tail_send)


def local(normed, cotangent, w_gate, w_up, w_down):
    _, length, depth = normed.shape
    width = w_gate.shape[2]
    chunks = width // CHUNK
    wide = (2 * CHUNK, CHUNK)
    anywhere = pl.BlockSpec(memory_space=pl.ANY)
    dma = pltpu.SemaphoreType.DMA
    passed, *grads = pl.pallas_call(
        kernel,
        out_shape=(pltpu.VMEM((1, depth, length), BF16), *[pltpu.VMEM(w_gate.shape, BF16)] * 3),
        in_specs=[anywhere] * 5,
        out_specs=(pl.BlockSpec(memory_space=pltpu.VMEM),) * 4,
        scratch_shapes=[
            pltpu.VMEM((2, depth, length), BF16),
            pltpu.VMEM((2, 4, 2, length, depth), BF16),
            pltpu.VMEM((2, depth, 8 * length), BF16),
            pltpu.VMEM((chunks, depth, 3 * CHUNK), BF16),
            *[pltpu.VMEM((chunks, 4, 2, length, w), BF16) for w in wide],
            *[pltpu.VMEM((chunks, 7, length, w), BF16) for w in wide],
            *[pltpu.VMEM((chunks, 4, 2, length, w), BF16) for w in wide],
            pltpu.VMEM((4, 2, length, depth), F32),
            pltpu.VMEM((8, length, depth), BF16),
            pltpu.VMEM((length, depth), BF16),
            dma((2,)),
            dma((chunks, 2)),
            dma((2, 4)),
            dma((2,)),
            dma((2, chunks, 6)),
            dma((2, 2, chunks)),
            dma(()),
            dma(()),
            dma(()),
            dma(()),
        ],
        compiler_params=pltpu.CompilerParams(
            collective_id=0, has_side_effects=True, vmem_limit_bytes=58_800_000
        ),
        name="geglu_relay",
    )(jnp.swapaxes(normed, 1, 2), jnp.swapaxes(cotangent, 1, 2), w_gate, w_up, w_down)
    return (jnp.swapaxes(passed, 1, 2), *grads)


def solution(mesh):
    in_specs = (
        P("section", "tp", "fsdp"),
        P("section", "tp", "fsdp"),
        P("section", "fsdp", "tp"),
        P("section", "fsdp", "tp"),
        P("section", "fsdp", "tp"),
    )
    out_specs = (
        P("section", "tp", "fsdp"),
        P("section", "fsdp", "tp"),
        P("section", "fsdp", "tp"),
        P("section", "fsdp", "tp"),
    )
    return jax.shard_map(local, mesh=mesh, in_specs=in_specs, out_specs=out_specs, check_vma=False)
```

```python
import functools
import math

import jax
import jax.numpy as jnp
from jax import lax
from jax.experimental import pallas as pl
from jax.experimental.pallas import tpu as pltpu
from jax.sharding import PartitionSpec as P

MESH = pl.DeviceIdType.MESH
CHUNK = 256
SUMS_Z = (2, 4, 5, 6)
SPREADS_Z = (0, 1, 7)
LAGS = {
    (0, 0): (0, 0),
    (0, 1): (20, 4),
    (0, 2): (27, 22),
    (0, 3): (46, 46),
    (0, 4): (81, 79),
    (0, 5): (84, 84),
    (0, 6): (90, 89),
    (1, 0): (6, 6),
    (1, 1): (28, 12),
    (1, 2): (40, 27),
    (1, 3): (84, 87),
    (1, 4): (90, 93),
    (1, 5): (96, 99),
    (1, 6): (105, 105),
}
ORDER = (
    (1, 1),
    (1, 6),
    (1, 5),
    (1, 0),
    (1, 2),
    (1, 3),
    (1, 4),
    (0, 0),
    (0, 3),
    (0, 1),
    (0, 2),
    (0, 6),
    (0, 4),
    (0, 5),
)
HEAD_AT = 4
BACK_AT = 6
LAST = 105
F32 = jnp.float32
BF16 = jnp.bfloat16


def activate(gate, up, back):
    coeff = math.sqrt(2.0 / math.pi)
    inner = jnp.tanh(coeff * (gate + 0.044715 * gate * gate * gate))
    act = 0.5 * gate * (1.0 + inner)
    slope = 0.5 * (1.0 + inner) + 0.5 * gate * (1.0 - inner * inner) * coeff * (
        1.0 + 3.0 * 0.044715 * gate * gate
    )
    return act * up, back * up * slope, back * act


def among(c, members):
    return functools.reduce(jnp.logical_or, [c == m for m in members])


def kernel(
    n_hbm, c_hbm, wg_hbm, wu_hbm, wd_hbm,
    passed, grad_gate, grad_up, grad_down,
    own, rows, rows_t, weights, part0, part1, arrived0, arrived1, grads0, grads1, branch,
    landed, other_cot,
    load_sem, weight_sem, head_sem, head_send, recv_sem, send_sem, tail_recv, tail_send, cot_sem, cot_send,
):
    parts, arriveds, gradss = (part0, part1), (arrived0, arrived1), (grads0, grads1)
    chunks = weights.shape[0]
    chunk = weights.shape[2] // 3
    depth = rows.shape[4]
    length = rows.shape[3]
    half = length // 2
    total = 8 * length
    low, high = pl.ds(0, half), pl.ds(half, half)
    columns = (pl.ds(0, 2 * chunk), pl.ds(2 * chunk, chunk))
    section = lax.axis_index("section")
    tp = lax.axis_index("tp")
    fsdp = lax.axis_index("fsdp")
    zl, x = tp // 4, tp % 4
    zh, y = fsdp // 4, fsdp % 4
    oz = 1 - zh
    ol = 1 - zl
    y1, y2, y3 = (y + 1) % 4, (y + 2) % 4, (y + 3) % 4
    x1, x2, x3 = (x + 1) % 4, (x + 2) % 4, (x + 3) % 4
    to_y1, to_y3 = ({"fsdp": zh * 4 + k} for k in (y1, y3))
    to_z = {"fsdp": oz * 4 + y}
    to_x1, to_x2, to_x3 = ({"tp": zl * 4 + k} for k in (x1, x2, x3))
    to_l = {"tp": ol * 4 + x}
    others = [{"section": 1 - section, "tp": t} for t in range(8)]

    loads = [pltpu.make_async_copy(hbm.at[0], own.at[k], load_sem.at[k]) for k, hbm in enumerate((n_hbm, c_hbm))]
    for load in loads:
        load.start()

    barrier = pltpu.get_barrier_semaphore()
    peers = [to_y1, to_y3, to_z, to_x1, to_x2, to_x3, to_l] + others
    for peer in peers:
        pl.semaphore_signal(barrier, inc=1, device_id=peer, device_id_type=MESH)

    def ready(k):
        loads[k].wait()
        rows[k, x, zl] = own[k].T

    ready(0)

    def send(src, dst, sender, recv, peer):
        pltpu.make_async_remote_copy(
            src_ref=src, dst_ref=dst, send_sem=sender, recv_sem=recv, device_id=peer, device_id_type=MESH
        ).start()

    def wait_for(ref, sem):
        pltpu.make_async_copy(ref, ref, sem).wait()

    def head(k, xx, ll, which, sem, *peers):
        ref = rows.at[k, xx, ll, which]
        for peer in peers:
            send(ref, ref, head_send.at[k], head_sem.at[k, sem], peer)

    def head_start(k):
        head(k, x, zl, high, 2, to_x1, to_x3, to_x2)
        head(k, x, zl, low, 0, to_l)
        head(k, x, zl, high, 3, to_l)
        head(k, x, zl, low, 1, to_x1, to_x3, to_x2)

    def head_middle(k):
        wait_for(rows.at[k, 0, 0, low], head_sem.at[k, 0])
        head(k, x, ol, low, 1, to_x1, to_x3, to_x2)
        wait_for(rows.at[k, 0:3, 0, low], head_sem.at[k, 2])
        for xx in (x1, x3, x2):
            head(k, xx, zl, high, 3, to_l)

    def head_end(k):
        wait_for(rows.at[k, 0:3, 0], head_sem.at[k, 1])
        wait_for(rows.at[k, 0:2, 0], head_sem.at[k, 3])

    pl.semaphore_wait(barrier, len(peers))
    head_start(0)

    for t in range(chunks):
        for k, hbm in enumerate((wg_hbm, wu_hbm, wd_hbm)):
            pltpu.make_async_copy(
                hbm.at[0, :, t * chunk : (t + 1) * chunk],
                weights.at[t, :, k * chunk : (k + 1) * chunk],
                weight_sem.at[t, k // 2],
            ).start()

    ready(1)
    head_middle(0)
    head_start(1)
    send(rows.at[1, x, zl], other_cot, cot_send, cot_sem, {"section": 1 - section})
    branch[...] = jnp.zeros_like(branch)
    head_end(0)

    def forward(s, c):
        wait_for(weights.at[c, :, columns[s]], weight_sem.at[c, s])

        def tile(k, _):
            left = rows[s, k].reshape(2 * length, depth)
            out = jnp.dot(left, weights[c, :, columns[s]], preferred_element_type=F32)
            parts[s][c, k] = out.astype(BF16).reshape(2, length, out.shape[1])
            return 0

        lax.fori_loop(0, 4, tile, 0)

    def add(dst, src):
        dst[...] = (dst[...].astype(F32) + src[...].astype(F32)).astype(BF16)

    def move(src, dst, s, c, k, *peers):
        for peer in peers:
            send(src, dst, send_sem.at[k // 3, s, c], recv_sem.at[s, c, k], peer)

    def sum_y(s, stage, c):
        part, arrived = parts[s].at[c], arriveds[s].at[c]
        if stage == 0:
            forward(s, c)
            move(part.at[y2, 0], arrived.at[0], s, c, 0, to_y1)
            move(part.at[y2, 1], arrived.at[1], s, c, 0, to_y3)
        elif stage == 1:
            wait_for(arrived.at[0:2], recv_sem.at[s, c, 0])
            add(part.at[y1, 0], arrived.at[0])
            move(part.at[y1], arrived.at[2:4], s, c, 1, to_y1)
            add(part.at[y3, 1], arrived.at[1])
            move(part.at[y3], arrived.at[4:6], s, c, 1, to_y3)
        else:
            wait_for(arrived.at[2:6], recv_sem.at[s, c, 1])
            part[y, oz] = (
                part[y, oz].astype(F32) + arrived[2 + oz].astype(F32) + arrived[4 + oz].astype(F32)
            ).astype(BF16)
            move(part.at[y, oz], arrived.at[6], s, c, 2, to_z)

    def sum_z(s, stage, c):
        part, arrived = parts[s].at[c], arriveds[s].at[c]
        if stage == 0:
            forward(s, c)
            for yy in (y2, y1, y3, y):
                move(part.at[yy, oz], arrived.at[yy], s, c, 0, to_z)
        elif stage == 1:
            wait_for(arrived.at[0:4], recv_sem.at[s, c, 0])
            add(part.at[y2, zh], arrived.at[y2])
            move(part.at[y2, zh, low], arrived.at[4, low], s, c, 1, to_y1)
            move(part.at[y2, zh, high], arrived.at[4, high], s, c, 1, to_y3)
            add(part.at[y1, zh], arrived.at[y1])
            add(part.at[y3, zh], arrived.at[y3])
        else:
            wait_for(arrived.at[4], recv_sem.at[s, c, 1])
            add(part.at[y1, zh, low], arrived.at[4, low])
            move(part.at[y1, zh], arrived.at[5], s, c, 2, to_y1)
            add(part.at[y3, zh, high], arrived.at[4, high])
            move(part.at[y3, zh], arrived.at[6], s, c, 2, to_y3)

    def final_y(s, c):
        wait_for(arriveds[s].at[c, 6], recv_sem.at[s, c, 2])
        return final(s, c, (2 + zh, 4 + zh, 6))

    def final_z(s, c):
        wait_for(arriveds[s].at[c, 5:7], recv_sem.at[s, c, 2])
        return final(s, c, (y, 5, 6))

    def final(s, c, terms):
        out = parts[s][c, y, zh].astype(F32)
        for t in terms:
            out = out + arriveds[s][c, t].astype(F32)
        return out

    def finish(c, done):
        gate_up, back = done(0, c), done(1, c)
        hidden, d_gate, d_up = activate(gate_up[:, :chunk], gate_up[:, chunk:], back)
        grads0[c, y, zh, :, :chunk] = d_gate.astype(BF16)
        grads0[c, y, zh, :, chunk:] = d_up.astype(BF16)
        grads1[c, y, zh] = hidden.astype(BF16)

    def spread(s, c, yy, zz, k, *peers, which=None):
        ref = gradss[s].at[c, yy, zz] if which is None else gradss[s].at[c, yy, zz, which]
        move(ref, ref, s, c, 3 + k, *peers)

    def spread_y(s, stage, c):
        grads = gradss[s].at[c]
        if stage == 0:
            spread(s, c, y, zh, 0, to_z)
            spread(s, c, y, zh, 1, to_y1, to_y3)
        elif stage == 1:
            wait_for(grads.at[0, 0], recv_sem.at[s, c, 3])
            spread(s, c, y, oz, 1, to_y1, to_y3)
        elif stage == 2:
            wait_for(grads.at[0:2], recv_sem.at[s, c, 4])
            spread(s, c, y3, 0, 2, to_y1)
            spread(s, c, y1, 1, 2, to_y3)
        else:
            wait_for(grads.at[0], recv_sem.at[s, c, 5])
            use(s, c)

    def spread_z(s, stage, c):
        grads = gradss[s].at[c]
        if stage == 0:
            spread(s, c, y, zh, 0, to_y1, to_y3)
            spread(s, c, y, zh, 2, to_z)
        elif stage == 1:
            wait_for(grads.at[0], recv_sem.at[s, c, 3])
            spread(s, c, y3, zh, 1, to_y1, which=low)
            spread(s, c, y1, zh, 1, to_y3, which=high)
            spread(s, c, y1, zh, 2, to_z)
            spread(s, c, y3, zh, 2, to_z)
        elif stage == 2:
            wait_for(grads.at[0, 0], recv_sem.at[s, c, 4])
            spread(s, c, y2, zh, 2, to_z)
        else:
            wait_for(grads.at[0:2], recv_sem.at[s, c, 5])
            use(s, c)

    def to_branch(c):
        def tile(k, _):
            back = lax.dot_general(
                grads0[c, k].reshape(2 * length, 2 * chunk),
                weights[c, :, columns[0]],
                (((1,), (1,)), ((), ())),
                preferred_element_type=F32,
            )
            branch[k] += back.reshape(2, length, depth)
            return 0

        lax.fori_loop(0, 4, tile, 0)

    def leave():
        for k in range(2):
            wait_for(landed.at[0:7], head_send.at[k])
        for r in range(8):
            rows[0, r // 2, r % 2] = branch[r // 2, r % 2].astype(BF16)
        for r in range(8):
            t = (r % 2) * 4 + r // 2
            send(rows.at[0, r // 2, r % 2], landed.at[tp], tail_send, tail_recv, others[t])

    def use(s, c):
        if s == 0:
            to_branch(c)
            pl.when(c == chunks - 1)(leave)
        m = depth // 3
        scale = 1.0 / math.sqrt(total)

        def tile(k, _):
            at = pl.ds(pl.multiple_of(k * m, m), m)
            right = gradss[s][c].reshape(total, gradss[s].shape[4])
            out = (jnp.dot(rows_t[s, at, :], right, preferred_element_type=F32) * scale).astype(BF16)
            for q, ref in enumerate(((grad_gate, grad_up), (grad_down,))[s]):
                ref[0, at, pl.ds(pl.multiple_of(c * chunk, chunk), chunk)] = out[:, q * chunk : (q + 1) * chunk]
            return 0

        lax.fori_loop(0, 3, tile, 0)

    def transposes():
        for k in range(2):
            for r in range(8):
                rows_t[k, :, r * length : (r + 1) * length] = rows[k, r // 2, r % 2].T

    def at_step(i, lags, members, for_y, for_z):
        for lag, what, z in zip(lags, (for_z, for_y), (True, False)):
            c = i - lag
            picked = among(c, members) if z else jnp.logical_not(among(c, members))

            @pl.when((c >= 0) & (c < chunks) & picked)
            def _():
                what(c)

    def step(i, _):
        pl.when(i == HEAD_AT)(functools.partial(head_middle, 1))

        @pl.when(i == BACK_AT)
        def _():
            head_end(1)

        for s, stage in ORDER:
            if stage < 3:
                bind = functools.partial
                at_step(i, LAGS[s, stage], SUMS_Z, bind(sum_y, s, stage), bind(sum_z, s, stage))
            else:
                if (s, stage) == (0, 3):
                    at_step(
                        i, LAGS[s, stage], SUMS_Z,
                        functools.partial(finish, done=final_y), functools.partial(finish, done=final_z),
                    )
                at_step(
                    i, LAGS[s, stage], SPREADS_Z,
                    functools.partial(spread_y, s, stage - 3), functools.partial(spread_z, s, stage - 3),
                )
        pl.when(i == BACK_AT + 1)(transposes)
        return 0

    lax.fori_loop(0, chunks + LAST, step, 0)

    wait_for(other_cot, cot_sem)
    wait_for(landed, tail_recv)
    summed = landed[0].astype(F32)
    for r in range(1, 8):
        summed = summed + landed[r].astype(F32)
    passed[0] = (other_cot[...].astype(F32) + summed).astype(BF16).T

    def drain(c, _):
        for k in range(2):
            for s in range(2):
                wait_for(arriveds[s].at[c], send_sem.at[k, s, c])
        return 0

    lax.fori_loop(0, chunks, drain, 0)
    wait_for(other_cot, cot_send)
    wait_for(rows.at[0], tail_send)


def local(normed, cotangent, w_gate, w_up, w_down):
    _, length, depth = normed.shape
    width = w_gate.shape[2]
    chunks = width // CHUNK
    wide = (2 * CHUNK, CHUNK)
    anywhere = pl.BlockSpec(memory_space=pl.ANY)
    dma = pltpu.SemaphoreType.DMA
    passed, *grads = pl.pallas_call(
        kernel,
        out_shape=(pltpu.VMEM((1, depth, length), BF16), *[pltpu.VMEM(w_gate.shape, BF16)] * 3),
        in_specs=[anywhere] * 5,
        out_specs=(pl.BlockSpec(memory_space=pltpu.VMEM),) * 4,
        scratch_shapes=[
            pltpu.VMEM((2, depth, length), BF16),
            pltpu.VMEM((2, 4, 2, length, depth), BF16),
            pltpu.VMEM((2, depth, 8 * length), BF16),
            pltpu.VMEM((chunks, depth, 3 * CHUNK), BF16),
            *[pltpu.VMEM((chunks, 4, 2, length, w), BF16) for w in wide],
            *[pltpu.VMEM((chunks, 7, length, w), BF16) for w in wide],
            *[pltpu.VMEM((chunks, 4, 2, length, w), BF16) for w in wide],
            pltpu.VMEM((4, 2, length, depth), F32),
            pltpu.VMEM((8, length, depth), BF16),
            pltpu.VMEM((length, depth), BF16),
            dma((2,)),
            dma((chunks, 2)),
            dma((2, 4)),
            dma((2,)),
            dma((2, chunks, 6)),
            dma((2, 2, chunks)),
            dma(()),
            dma(()),
            dma(()),
            dma(()),
        ],
        compiler_params=pltpu.CompilerParams(
            collective_id=0, has_side_effects=True, vmem_limit_bytes=58_800_000
        ),
        name="geglu_relay",
    )(jnp.swapaxes(normed, 1, 2), jnp.swapaxes(cotangent, 1, 2), w_gate, w_up, w_down)
    return (jnp.swapaxes(passed, 1, 2), *grads)


def solution(mesh):
    in_specs = (
        P("section", "tp", "fsdp"),
        P("section", "tp", "fsdp"),
        P("section", "fsdp", "tp"),
        P("section", "fsdp", "tp"),
        P("section", "fsdp", "tp"),
    )
    out_specs = (
        P("section", "tp", "fsdp"),
        P("section", "fsdp", "tp"),
        P("section", "fsdp", "tp"),
        P("section", "fsdp", "tp"),
    )
    return jax.shard_map(local, mesh=mesh, in_specs=in_specs, out_specs=out_specs, check_vma=False)
```

```python
import functools
import math

import jax
import jax.numpy as jnp
from jax import lax
from jax.experimental import pallas as pl
from jax.experimental.pallas import tpu as pltpu
from jax.sharding import PartitionSpec as P

MESH = pl.DeviceIdType.MESH
CHUNK = 256
SUMS_Z = (2, 4, 5, 6)
SPREADS_Z = (0, 1, 7)
LAGS = {
    (0, 0): (0, 0),
    (0, 1): (20, 4),
    (0, 2): (27, 22),
    (0, 3): (46, 46),
    (0, 4): (81, 79),
    (0, 5): (84, 84),
    (0, 6): (90, 89),
    (1, 0): (6, 6),
    (1, 1): (28, 12),
    (1, 2): (40, 27),
    (1, 3): (84, 87),
    (1, 4): (90, 93),
    (1, 5): (96, 99),
    (1, 6): (105, 105),
}
ORDER = (
    (1, 1),
    (1, 6),
    (1, 5),
    (1, 0),
    (1, 2),
    (1, 3),
    (1, 4),
    (0, 0),
    (0, 3),
    (0, 1),
    (0, 2),
    (0, 6),
    (0, 4),
    (0, 5),
)
HEAD_AT = 4
BACK_AT = 6
LAST = 105
F32 = jnp.float32
BF16 = jnp.bfloat16


def activate(gate, up, back):
    coeff = math.sqrt(2.0 / math.pi)
    inner = jnp.tanh(coeff * (gate + 0.044715 * gate * gate * gate))
    act = 0.5 * gate * (1.0 + inner)
    slope = 0.5 * (1.0 + inner) + 0.5 * gate * (1.0 - inner * inner) * coeff * (
        1.0 + 3.0 * 0.044715 * gate * gate
    )
    return act * up, back * up * slope, back * act


def among(c, members):
    return functools.reduce(jnp.logical_or, [c == m for m in members])


def kernel(
    n_hbm, c_hbm, wg_hbm, wu_hbm, wd_hbm,
    passed, grad_gate, grad_up, grad_down,
    own, rows, rows_t, weights, part0, part1, arrived0, arrived1, grads0, grads1, branch,
    landed, other_cot,
    load_sem, weight_sem, head_sem, head_send, recv_sem, send_sem, tail_recv, tail_send, cot_sem, cot_send,
):
    parts, arriveds, gradss = (part0, part1), (arrived0, arrived1), (grads0, grads1)
    chunks = weights.shape[0]
    chunk = weights.shape[2] // 3
    depth = rows.shape[4]
    length = rows.shape[3]
    half = length // 2
    total = 8 * length
    low, high, whole = pl.ds(0, half), pl.ds(half, half), pl.ds(0, length)
    columns = (pl.ds(0, 2 * chunk), pl.ds(2 * chunk, chunk))
    section = lax.axis_index("section")
    tp = lax.axis_index("tp")
    fsdp = lax.axis_index("fsdp")
    zl, x = tp // 4, tp % 4
    zh, y = fsdp // 4, fsdp % 4
    oz = 1 - zh
    ol = 1 - zl
    y1, y2, y3 = (y + 1) % 4, (y + 2) % 4, (y + 3) % 4
    x1, x2, x3 = (x + 1) % 4, (x + 2) % 4, (x + 3) % 4
    to_y1, to_y3 = ({"fsdp": zh * 4 + k} for k in (y1, y3))
    to_z = {"fsdp": oz * 4 + y}
    to_x1, to_x2, to_x3 = ({"tp": zl * 4 + k} for k in (x1, x2, x3))
    to_l = {"tp": ol * 4 + x}
    others = [{"section": 1 - section, "tp": t} for t in range(8)]

    loads = [pltpu.make_async_copy(hbm.at[0], own.at[k], load_sem.at[k]) for k, hbm in enumerate((n_hbm, c_hbm))]
    for load in loads:
        load.start()

    barrier = pltpu.get_barrier_semaphore()
    peers = [to_y1, to_y3, to_z, to_x1, to_x2, to_x3, to_l] + others
    for peer in peers:
        pl.semaphore_signal(barrier, inc=1, device_id=peer, device_id_type=MESH)

    def ready(k):
        loads[k].wait()
        rows[k, x, zl] = own[k].T

    ready(0)

    def send(src, dst, sender, recv, peer):
        pltpu.make_async_remote_copy(
            src_ref=src, dst_ref=dst, send_sem=sender, recv_sem=recv, device_id=peer, device_id_type=MESH
        ).start()

    def wait_for(ref, sem):
        pltpu.make_async_copy(ref, ref, sem).wait()

    def head(k, xx, ll, which, sem, *peers):
        ref = rows.at[k, xx, ll, which]
        for peer in peers:
            send(ref, ref, head_send.at[k], head_sem.at[k, sem], peer)

    def head_start(k):
        head(k, x, zl, high, 2, to_x1, to_x3, to_x2)
        head(k, x, zl, low, 0, to_l)
        head(k, x, zl, high, 3, to_l)
        head(k, x, zl, low, 1, to_x1, to_x3, to_x2)

    def head_middle(k):
        wait_for(rows.at[k, 0, 0, low], head_sem.at[k, 0])
        head(k, x, ol, low, 1, to_x1, to_x3, to_x2)
        wait_for(rows.at[k, 0:3, 0, low], head_sem.at[k, 2])
        for xx in (x1, x3, x2):
            head(k, xx, zl, high, 3, to_l)

    def cot_start():
        head(1, x, zl, whole, 0, to_l)
        head(1, x, zl, whole, 1, to_x1, to_x3, to_x2)

    def cot_middle():
        wait_for(rows.at[1, 0, 0], head_sem.at[1, 0])
        head(1, x, ol, whole, 1, to_x1, to_x3, to_x2)

    def cot_end():
        wait_for(rows.at[1, 0:3], head_sem.at[1, 1])

    def head_end(k):
        wait_for(rows.at[k, 0:3, 0], head_sem.at[k, 1])
        wait_for(rows.at[k, 0:2, 0], head_sem.at[k, 3])

    pl.semaphore_wait(barrier, len(peers))
    head_start(0)

    for t in range(chunks):
        for k, hbm in enumerate((wg_hbm, wu_hbm, wd_hbm)):
            pltpu.make_async_copy(
                hbm.at[0, :, t * chunk : (t + 1) * chunk],
                weights.at[t, :, k * chunk : (k + 1) * chunk],
                weight_sem.at[t, k // 2],
            ).start()

    ready(1)
    head_middle(0)
    cot_start()
    send(rows.at[1, x, zl], other_cot, cot_send, cot_sem, {"section": 1 - section})
    branch[...] = jnp.zeros_like(branch)
    head_end(0)

    def forward(s, c):
        wait_for(weights.at[c, :, columns[s]], weight_sem.at[c, s])

        def tile(k, _):
            left = rows[s, k].reshape(2 * length, depth)
            out = jnp.dot(left, weights[c, :, columns[s]], preferred_element_type=F32)
            parts[s][c, k] = out.astype(BF16).reshape(2, length, out.shape[1])
            return 0

        lax.fori_loop(0, 4, tile, 0)

    def add(dst, src):
        dst[...] = (dst[...].astype(F32) + src[...].astype(F32)).astype(BF16)

    def move(src, dst, s, c, k, *peers):
        for peer in peers:
            send(src, dst, send_sem.at[k // 3, s, c], recv_sem.at[s, c, k], peer)

    def sum_y(s, stage, c):
        part, arrived = parts[s].at[c], arriveds[s].at[c]
        if stage == 0:
            forward(s, c)
            move(part.at[y2, 0], arrived.at[0], s, c, 0, to_y1)
            move(part.at[y2, 1], arrived.at[1], s, c, 0, to_y3)
        elif stage == 1:
            wait_for(arrived.at[0:2], recv_sem.at[s, c, 0])
            add(part.at[y1, 0], arrived.at[0])
            move(part.at[y1], arrived.at[2:4], s, c, 1, to_y1)
            add(part.at[y3, 1], arrived.at[1])
            move(part.at[y3], arrived.at[4:6], s, c, 1, to_y3)
        else:
            wait_for(arrived.at[2:6], recv_sem.at[s, c, 1])
            part[y, oz] = (
                part[y, oz].astype(F32) + arrived[2 + oz].astype(F32) + arrived[4 + oz].astype(F32)
            ).astype(BF16)
            move(part.at[y, oz], arrived.at[6], s, c, 2, to_z)

    def sum_z(s, stage, c):
        part, arrived = parts[s].at[c], arriveds[s].at[c]
        if stage == 0:
            forward(s, c)
            for yy in (y2, y1, y3, y):
                move(part.at[yy, oz], arrived.at[yy], s, c, 0, to_z)
        elif stage == 1:
            wait_for(arrived.at[0:4], recv_sem.at[s, c, 0])
            add(part.at[y2, zh], arrived.at[y2])
            move(part.at[y2, zh, low], arrived.at[4, low], s, c, 1, to_y1)
            move(part.at[y2, zh, high], arrived.at[4, high], s, c, 1, to_y3)
            add(part.at[y1, zh], arrived.at[y1])
            add(part.at[y3, zh], arrived.at[y3])
        else:
            wait_for(arrived.at[4], recv_sem.at[s, c, 1])
            add(part.at[y1, zh, low], arrived.at[4, low])
            move(part.at[y1, zh], arrived.at[5], s, c, 2, to_y1)
            add(part.at[y3, zh, high], arrived.at[4, high])
            move(part.at[y3, zh], arrived.at[6], s, c, 2, to_y3)

    def final_y(s, c):
        wait_for(arriveds[s].at[c, 6], recv_sem.at[s, c, 2])
        return final(s, c, (2 + zh, 4 + zh, 6))

    def final_z(s, c):
        wait_for(arriveds[s].at[c, 5:7], recv_sem.at[s, c, 2])
        return final(s, c, (y, 5, 6))

    def final(s, c, terms):
        out = parts[s][c, y, zh].astype(F32)
        for t in terms:
            out = out + arriveds[s][c, t].astype(F32)
        return out

    def finish(c, done):
        gate_up, back = done(0, c), done(1, c)
        hidden, d_gate, d_up = activate(gate_up[:, :chunk], gate_up[:, chunk:], back)
        grads0[c, y, zh, :, :chunk] = d_gate.astype(BF16)
        grads0[c, y, zh, :, chunk:] = d_up.astype(BF16)
        grads1[c, y, zh] = hidden.astype(BF16)

    def spread(s, c, yy, zz, k, *peers, which=None):
        ref = gradss[s].at[c, yy, zz] if which is None else gradss[s].at[c, yy, zz, which]
        move(ref, ref, s, c, 3 + k, *peers)

    def spread_y(s, stage, c):
        grads = gradss[s].at[c]
        if stage == 0:
            spread(s, c, y, zh, 0, to_z)
            spread(s, c, y, zh, 1, to_y1, to_y3)
        elif stage == 1:
            wait_for(grads.at[0, 0], recv_sem.at[s, c, 3])
            spread(s, c, y, oz, 1, to_y1, to_y3)
        elif stage == 2:
            wait_for(grads.at[0:2], recv_sem.at[s, c, 4])
            spread(s, c, y3, 0, 2, to_y1)
            spread(s, c, y1, 1, 2, to_y3)
        else:
            wait_for(grads.at[0], recv_sem.at[s, c, 5])
            use(s, c)

    def spread_z(s, stage, c):
        grads = gradss[s].at[c]
        if stage == 0:
            spread(s, c, y, zh, 0, to_y1, to_y3)
            spread(s, c, y, zh, 2, to_z)
        elif stage == 1:
            wait_for(grads.at[0], recv_sem.at[s, c, 3])
            spread(s, c, y3, zh, 1, to_y1, which=low)
            spread(s, c, y1, zh, 1, to_y3, which=high)
            spread(s, c, y1, zh, 2, to_z)
            spread(s, c, y3, zh, 2, to_z)
        elif stage == 2:
            wait_for(grads.at[0, 0], recv_sem.at[s, c, 4])
            spread(s, c, y2, zh, 2, to_z)
        else:
            wait_for(grads.at[0:2], recv_sem.at[s, c, 5])
            use(s, c)

    def to_branch(c):
        def tile(k, _):
            back = lax.dot_general(
                grads0[c, k].reshape(2 * length, 2 * chunk),
                weights[c, :, columns[0]],
                (((1,), (1,)), ((), ())),
                preferred_element_type=F32,
            )
            branch[k] += back.reshape(2, length, depth)
            return 0

        lax.fori_loop(0, 4, tile, 0)

    def leave():
        for k in range(2):
            wait_for(landed.at[0:7], head_send.at[k])
        for r in range(8):
            rows[0, r // 2, r % 2] = branch[r // 2, r % 2].astype(BF16)
        for r in range(8):
            t = (r % 2) * 4 + r // 2
            send(rows.at[0, r // 2, r % 2], landed.at[tp], tail_send, tail_recv, others[t])

    def use(s, c):
        if s == 0:
            to_branch(c)
            pl.when(c == chunks - 1)(leave)
        m = depth // 3
        scale = 1.0 / math.sqrt(total)

        def tile(k, _):
            at = pl.ds(pl.multiple_of(k * m, m), m)
            right = gradss[s][c].reshape(total, gradss[s].shape[4])
            out = (jnp.dot(rows_t[s, at, :], right, preferred_element_type=F32) * scale).astype(BF16)
            for q, ref in enumerate(((grad_gate, grad_up), (grad_down,))[s]):
                ref[0, at, pl.ds(pl.multiple_of(c * chunk, chunk), chunk)] = out[:, q * chunk : (q + 1) * chunk]
            return 0

        lax.fori_loop(0, 3, tile, 0)

    def transposes():
        for k in range(2):
            for r in range(8):
                rows_t[k, :, r * length : (r + 1) * length] = rows[k, r // 2, r % 2].T

    def at_step(i, lags, members, for_y, for_z):
        for lag, what, z in zip(lags, (for_z, for_y), (True, False)):
            c = i - lag
            picked = among(c, members) if z else jnp.logical_not(among(c, members))

            @pl.when((c >= 0) & (c < chunks) & picked)
            def _():
                what(c)

    def step(i, _):
        pl.when(i == HEAD_AT)(cot_middle)

        pl.when(i == BACK_AT)(cot_end)

        for s, stage in ORDER:
            if stage < 3:
                bind = functools.partial
                at_step(i, LAGS[s, stage], SUMS_Z, bind(sum_y, s, stage), bind(sum_z, s, stage))
            else:
                if (s, stage) == (0, 3):
                    at_step(
                        i, LAGS[s, stage], SUMS_Z,
                        functools.partial(finish, done=final_y), functools.partial(finish, done=final_z),
                    )
                at_step(
                    i, LAGS[s, stage], SPREADS_Z,
                    functools.partial(spread_y, s, stage - 3), functools.partial(spread_z, s, stage - 3),
                )
        pl.when(i == BACK_AT + 1)(transposes)
        return 0

    lax.fori_loop(0, chunks + LAST, step, 0)

    wait_for(other_cot, cot_sem)
    wait_for(landed, tail_recv)
    summed = landed[0].astype(F32)
    for r in range(1, 8):
        summed = summed + landed[r].astype(F32)
    passed[0] = (other_cot[...].astype(F32) + summed).astype(BF16).T

    def drain(c, _):
        for k in range(2):
            for s in range(2):
                wait_for(arriveds[s].at[c], send_sem.at[k, s, c])
        return 0

    lax.fori_loop(0, chunks, drain, 0)
    wait_for(other_cot, cot_send)
    wait_for(rows.at[0], tail_send)


def local(normed, cotangent, w_gate, w_up, w_down):
    _, length, depth = normed.shape
    width = w_gate.shape[2]
    chunks = width // CHUNK
    wide = (2 * CHUNK, CHUNK)
    anywhere = pl.BlockSpec(memory_space=pl.ANY)
    dma = pltpu.SemaphoreType.DMA
    passed, *grads = pl.pallas_call(
        kernel,
        out_shape=(pltpu.VMEM((1, depth, length), BF16), *[pltpu.VMEM(w_gate.shape, BF16)] * 3),
        in_specs=[anywhere] * 5,
        out_specs=(pl.BlockSpec(memory_space=pltpu.VMEM),) * 4,
        scratch_shapes=[
            pltpu.VMEM((2, depth, length), BF16),
            pltpu.VMEM((2, 4, 2, length, depth), BF16),
            pltpu.VMEM((2, depth, 8 * length), BF16),
            pltpu.VMEM((chunks, depth, 3 * CHUNK), BF16),
            *[pltpu.VMEM((chunks, 4, 2, length, w), BF16) for w in wide],
            *[pltpu.VMEM((chunks, 7, length, w), BF16) for w in wide],
            *[pltpu.VMEM((chunks, 4, 2, length, w), BF16) for w in wide],
            pltpu.VMEM((4, 2, length, depth), F32),
            pltpu.VMEM((8, length, depth), BF16),
            pltpu.VMEM((length, depth), BF16),
            dma((2,)),
            dma((chunks, 2)),
            dma((2, 4)),
            dma((2,)),
            dma((2, chunks, 6)),
            dma((2, 2, chunks)),
            dma(()),
            dma(()),
            dma(()),
            dma(()),
        ],
        compiler_params=pltpu.CompilerParams(
            collective_id=0, has_side_effects=True, vmem_limit_bytes=58_800_000
        ),
        name="geglu_relay",
    )(jnp.swapaxes(normed, 1, 2), jnp.swapaxes(cotangent, 1, 2), w_gate, w_up, w_down)
    return (jnp.swapaxes(passed, 1, 2), *grads)


def solution(mesh):
    in_specs = (
        P("section", "tp", "fsdp"),
        P("section", "tp", "fsdp"),
        P("section", "fsdp", "tp"),
        P("section", "fsdp", "tp"),
        P("section", "fsdp", "tp"),
    )
    out_specs = (
        P("section", "tp", "fsdp"),
        P("section", "fsdp", "tp"),
        P("section", "fsdp", "tp"),
        P("section", "fsdp", "tp"),
    )
    return jax.shard_map(local, mesh=mesh, in_specs=in_specs, out_specs=out_specs, check_vma=False)
```

```python
import functools
import math

import jax
import jax.numpy as jnp
from jax import lax
from jax.experimental import pallas as pl
from jax.experimental.pallas import tpu as pltpu
from jax.sharding import PartitionSpec as P

MESH = pl.DeviceIdType.MESH
CHUNK = 256
SUMS_Z = (2, 4, 5, 6)
SPREADS_Z = (0, 1, 7)
LAGS = {
    (0, 0): (0, 0),
    (0, 1): (20, 4),
    (0, 2): (27, 22),
    (0, 3): (46, 46),
    (0, 4): (81, 79),
    (0, 5): (84, 84),
    (0, 6): (90, 89),
    (1, 0): (6, 6),
    (1, 1): (28, 12),
    (1, 2): (40, 27),
    (1, 3): (84, 87),
    (1, 4): (90, 93),
    (1, 5): (96, 99),
    (1, 6): (105, 105),
}
ORDER = (
    (1, 1),
    (1, 6),
    (1, 5),
    (1, 0),
    (1, 2),
    (1, 3),
    (1, 4),
    (0, 0),
    (0, 3),
    (0, 1),
    (0, 2),
    (0, 6),
    (0, 4),
    (0, 5),
)
HEAD_AT = 1
BACK_AT = 6
LAST = 105
F32 = jnp.float32
BF16 = jnp.bfloat16


def activate(gate, up, back):
    coeff = math.sqrt(2.0 / math.pi)
    inner = jnp.tanh(coeff * (gate + 0.044715 * gate * gate * gate))
    act = 0.5 * gate * (1.0 + inner)
    slope = 0.5 * (1.0 + inner) + 0.5 * gate * (1.0 - inner * inner) * coeff * (
        1.0 + 3.0 * 0.044715 * gate * gate
    )
    return act * up, back * up * slope, back * act


def among(c, members):
    return functools.reduce(jnp.logical_or, [c == m for m in members])


def kernel(
    n_hbm, c_hbm, wg_hbm, wu_hbm, wd_hbm,
    passed, grad_gate, grad_up, grad_down,
    own, rows, rows_t, weights, part0, part1, arrived0, arrived1, grads0, grads1, branch,
    landed, other_cot,
    load_sem, weight_sem, head_sem, head_send, recv_sem, send_sem, tail_recv, tail_send, cot_sem, cot_send,
):
    parts, arriveds, gradss = (part0, part1), (arrived0, arrived1), (grads0, grads1)
    chunks = weights.shape[0]
    chunk = weights.shape[2] // 3
    depth = rows.shape[4]
    length = rows.shape[3]
    half = length // 2
    total = 8 * length
    low, high, whole = pl.ds(0, half), pl.ds(half, half), pl.ds(0, length)
    columns = (pl.ds(0, 2 * chunk), pl.ds(2 * chunk, chunk))
    section = lax.axis_index("section")
    tp = lax.axis_index("tp")
    fsdp = lax.axis_index("fsdp")
    zl, x = tp // 4, tp % 4
    zh, y = fsdp // 4, fsdp % 4
    oz = 1 - zh
    ol = 1 - zl
    y1, y2, y3 = (y + 1) % 4, (y + 2) % 4, (y + 3) % 4
    x1, x2, x3 = (x + 1) % 4, (x + 2) % 4, (x + 3) % 4
    to_y1, to_y3 = ({"fsdp": zh * 4 + k} for k in (y1, y3))
    to_z = {"fsdp": oz * 4 + y}
    to_x1, to_x2, to_x3 = ({"tp": zl * 4 + k} for k in (x1, x2, x3))
    to_l = {"tp": ol * 4 + x}
    others = [{"section": 1 - section, "tp": t} for t in range(8)]

    loads = [pltpu.make_async_copy(hbm.at[0], own.at[k], load_sem.at[k]) for k, hbm in enumerate((n_hbm, c_hbm))]
    for load in loads:
        load.start()

    barrier = pltpu.get_barrier_semaphore()
    peers = [to_y1, to_y3, to_z, to_x1, to_x2, to_x3, to_l] + others
    for peer in peers:
        pl.semaphore_signal(barrier, inc=1, device_id=peer, device_id_type=MESH)

    def ready(k):
        loads[k].wait()
        rows[k, x, zl] = own[k].T

    ready(0)

    def send(src, dst, sender, recv, peer):
        pltpu.make_async_remote_copy(
            src_ref=src, dst_ref=dst, send_sem=sender, recv_sem=recv, device_id=peer, device_id_type=MESH
        ).start()

    def wait_for(ref, sem):
        pltpu.make_async_copy(ref, ref, sem).wait()

    def head(k, xx, ll, which, sem, *peers):
        ref = rows.at[k, xx, ll, which]
        for peer in peers:
            send(ref, ref, head_send.at[k], head_sem.at[k, sem], peer)

    def head_start(k):
        head(k, x, zl, high, 2, to_x1, to_x3, to_x2)
        head(k, x, zl, low, 0, to_l)
        head(k, x, zl, high, 3, to_l)
        head(k, x, zl, low, 1, to_x1, to_x3, to_x2)

    def head_middle(k):
        wait_for(rows.at[k, 0, 0, low], head_sem.at[k, 0])
        head(k, x, ol, low, 1, to_x1, to_x3, to_x2)
        wait_for(rows.at[k, 0:3, 0, low], head_sem.at[k, 2])
        for xx in (x1, x3, x2):
            head(k, xx, zl, high, 3, to_l)

    def cot_start():
        head(1, x, zl, whole, 0, to_l)
        head(1, x, zl, whole, 1, to_x1, to_x3, to_x2)

    def cot_middle():
        wait_for(rows.at[1, 0, 0], head_sem.at[1, 0])
        head(1, x, ol, whole, 1, to_x1, to_x3, to_x2)

    def cot_end():
        wait_for(rows.at[1, 0:3], head_sem.at[1, 1])

    def head_end(k):
        wait_for(rows.at[k, 0:3, 0], head_sem.at[k, 1])
        wait_for(rows.at[k, 0:2, 0], head_sem.at[k, 3])

    pl.semaphore_wait(barrier, len(peers))
    head_start(0)

    for t in range(chunks):
        for k, hbm in enumerate((wg_hbm, wu_hbm, wd_hbm)):
            pltpu.make_async_copy(
                hbm.at[0, :, t * chunk : (t + 1) * chunk],
                weights.at[t, :, k * chunk : (k + 1) * chunk],
                weight_sem.at[t, k // 2],
            ).start()

    ready(1)
    head_middle(0)
    cot_start()
    send(rows.at[1, x, zl], other_cot, cot_send, cot_sem, {"section": 1 - section})
    branch[...] = jnp.zeros_like(branch)
    head_end(0)

    def forward(s, c):
        wait_for(weights.at[c, :, columns[s]], weight_sem.at[c, s])

        def tile(k, _):
            left = rows[s, k].reshape(2 * length, depth)
            out = jnp.dot(left, weights[c, :, columns[s]], preferred_element_type=F32)
            parts[s][c, k] = out.astype(BF16).reshape(2, length, out.shape[1])
            return 0

        lax.fori_loop(0, 4, tile, 0)

    def add(dst, src):
        dst[...] = (dst[...].astype(F32) + src[...].astype(F32)).astype(BF16)

    def move(src, dst, s, c, k, *peers):
        for peer in peers:
            send(src, dst, send_sem.at[k // 3, s, c], recv_sem.at[s, c, k], peer)

    def sum_y(s, stage, c):
        part, arrived = parts[s].at[c], arriveds[s].at[c]
        if stage == 0:
            forward(s, c)
            move(part.at[y2, 0], arrived.at[0], s, c, 0, to_y1)
            move(part.at[y2, 1], arrived.at[1], s, c, 0, to_y3)
        elif stage == 1:
            wait_for(arrived.at[0:2], recv_sem.at[s, c, 0])
            add(part.at[y1, 0], arrived.at[0])
            move(part.at[y1], arrived.at[2:4], s, c, 1, to_y1)
            add(part.at[y3, 1], arrived.at[1])
            move(part.at[y3], arrived.at[4:6], s, c, 1, to_y3)
        else:
            wait_for(arrived.at[2:6], recv_sem.at[s, c, 1])
            part[y, oz] = (
                part[y, oz].astype(F32) + arrived[2 + oz].astype(F32) + arrived[4 + oz].astype(F32)
            ).astype(BF16)
            move(part.at[y, oz], arrived.at[6], s, c, 2, to_z)

    def sum_z(s, stage, c):
        part, arrived = parts[s].at[c], arriveds[s].at[c]
        if stage == 0:
            forward(s, c)
            for yy in (y2, y1, y3, y):
                move(part.at[yy, oz], arrived.at[yy], s, c, 0, to_z)
        elif stage == 1:
            wait_for(arrived.at[0:4], recv_sem.at[s, c, 0])
            add(part.at[y2, zh], arrived.at[y2])
            move(part.at[y2, zh, low], arrived.at[4, low], s, c, 1, to_y1)
            move(part.at[y2, zh, high], arrived.at[4, high], s, c, 1, to_y3)
            add(part.at[y1, zh], arrived.at[y1])
            add(part.at[y3, zh], arrived.at[y3])
        else:
            wait_for(arrived.at[4], recv_sem.at[s, c, 1])
            add(part.at[y1, zh, low], arrived.at[4, low])
            move(part.at[y1, zh], arrived.at[5], s, c, 2, to_y1)
            add(part.at[y3, zh, high], arrived.at[4, high])
            move(part.at[y3, zh], arrived.at[6], s, c, 2, to_y3)

    def final_y(s, c):
        wait_for(arriveds[s].at[c, 6], recv_sem.at[s, c, 2])
        return final(s, c, (2 + zh, 4 + zh, 6))

    def final_z(s, c):
        wait_for(arriveds[s].at[c, 5:7], recv_sem.at[s, c, 2])
        return final(s, c, (y, 5, 6))

    def final(s, c, terms):
        out = parts[s][c, y, zh].astype(F32)
        for t in terms:
            out = out + arriveds[s][c, t].astype(F32)
        return out

    def finish(c, done):
        gate_up, back = done(0, c), done(1, c)
        hidden, d_gate, d_up = activate(gate_up[:, :chunk], gate_up[:, chunk:], back)
        grads0[c, y, zh, :, :chunk] = d_gate.astype(BF16)
        grads0[c, y, zh, :, chunk:] = d_up.astype(BF16)
        grads1[c, y, zh] = hidden.astype(BF16)

    def spread(s, c, yy, zz, k, *peers, which=None):
        ref = gradss[s].at[c, yy, zz] if which is None else gradss[s].at[c, yy, zz, which]
        move(ref, ref, s, c, 3 + k, *peers)

    def spread_y(s, stage, c):
        grads = gradss[s].at[c]
        if stage == 0:
            spread(s, c, y, zh, 0, to_z)
            spread(s, c, y, zh, 1, to_y1, to_y3)
        elif stage == 1:
            wait_for(grads.at[0, 0], recv_sem.at[s, c, 3])
            spread(s, c, y, oz, 1, to_y1, to_y3)
        elif stage == 2:
            wait_for(grads.at[0:2], recv_sem.at[s, c, 4])
            spread(s, c, y3, 0, 2, to_y1)
            spread(s, c, y1, 1, 2, to_y3)
        else:
            wait_for(grads.at[0], recv_sem.at[s, c, 5])
            use(s, c)

    def spread_z(s, stage, c):
        grads = gradss[s].at[c]
        if stage == 0:
            spread(s, c, y, zh, 0, to_y1, to_y3)
            spread(s, c, y, zh, 2, to_z)
        elif stage == 1:
            wait_for(grads.at[0], recv_sem.at[s, c, 3])
            spread(s, c, y3, zh, 1, to_y1, which=low)
            spread(s, c, y1, zh, 1, to_y3, which=high)
            spread(s, c, y1, zh, 2, to_z)
            spread(s, c, y3, zh, 2, to_z)
        elif stage == 2:
            wait_for(grads.at[0, 0], recv_sem.at[s, c, 4])
            spread(s, c, y2, zh, 2, to_z)
        else:
            wait_for(grads.at[0:2], recv_sem.at[s, c, 5])
            use(s, c)

    def to_branch(c):
        def tile(k, _):
            back = lax.dot_general(
                grads0[c, k].reshape(2 * length, 2 * chunk),
                weights[c, :, columns[0]],
                (((1,), (1,)), ((), ())),
                preferred_element_type=F32,
            )
            branch[k] += back.reshape(2, length, depth)
            return 0

        lax.fori_loop(0, 4, tile, 0)

    def leave():
        for k in range(2):
            wait_for(landed.at[0:7], head_send.at[k])
        for r in range(8):
            rows[0, r // 2, r % 2] = branch[r // 2, r % 2].astype(BF16)
        for r in range(8):
            t = (r % 2) * 4 + r // 2
            send(rows.at[0, r // 2, r % 2], landed.at[tp], tail_send, tail_recv, others[t])

    def use(s, c):
        if s == 0:
            to_branch(c)
            pl.when(c == chunks - 1)(leave)
        m = depth // 3
        scale = 1.0 / math.sqrt(total)

        def tile(k, _):
            at = pl.ds(pl.multiple_of(k * m, m), m)
            right = gradss[s][c].reshape(total, gradss[s].shape[4])
            out = (jnp.dot(rows_t[s, at, :], right, preferred_element_type=F32) * scale).astype(BF16)
            for q, ref in enumerate(((grad_gate, grad_up), (grad_down,))[s]):
                ref[0, at, pl.ds(pl.multiple_of(c * chunk, chunk), chunk)] = out[:, q * chunk : (q + 1) * chunk]
            return 0

        lax.fori_loop(0, 3, tile, 0)

    def transposes():
        for k in range(2):
            for r in range(8):
                rows_t[k, :, r * length : (r + 1) * length] = rows[k, r // 2, r % 2].T

    def at_step(i, lags, members, for_y, for_z):
        for lag, what, z in zip(lags, (for_z, for_y), (True, False)):
            c = i - lag
            picked = among(c, members) if z else jnp.logical_not(among(c, members))

            @pl.when((c >= 0) & (c < chunks) & picked)
            def _():
                what(c)

    def step(i, _):
        pl.when(i == HEAD_AT)(cot_middle)

        pl.when(i == BACK_AT)(cot_end)

        for s, stage in ORDER:
            if stage < 3:
                bind = functools.partial
                at_step(i, LAGS[s, stage], SUMS_Z, bind(sum_y, s, stage), bind(sum_z, s, stage))
            else:
                if (s, stage) == (0, 3):
                    at_step(
                        i, LAGS[s, stage], SUMS_Z,
                        functools.partial(finish, done=final_y), functools.partial(finish, done=final_z),
                    )
                at_step(
                    i, LAGS[s, stage], SPREADS_Z,
                    functools.partial(spread_y, s, stage - 3), functools.partial(spread_z, s, stage - 3),
                )
        pl.when(i == BACK_AT + 1)(transposes)
        return 0

    lax.fori_loop(0, chunks + LAST, step, 0)

    wait_for(other_cot, cot_sem)
    wait_for(landed, tail_recv)
    summed = landed[0].astype(F32)
    for r in range(1, 8):
        summed = summed + landed[r].astype(F32)
    passed[0] = (other_cot[...].astype(F32) + summed).astype(BF16).T

    def drain(c, _):
        for k in range(2):
            for s in range(2):
                wait_for(arriveds[s].at[c], send_sem.at[k, s, c])
        return 0

    lax.fori_loop(0, chunks, drain, 0)
    wait_for(other_cot, cot_send)
    wait_for(rows.at[0], tail_send)


def local(normed, cotangent, w_gate, w_up, w_down):
    _, length, depth = normed.shape
    width = w_gate.shape[2]
    chunks = width // CHUNK
    wide = (2 * CHUNK, CHUNK)
    anywhere = pl.BlockSpec(memory_space=pl.ANY)
    dma = pltpu.SemaphoreType.DMA
    passed, *grads = pl.pallas_call(
        kernel,
        out_shape=(pltpu.VMEM((1, depth, length), BF16), *[pltpu.VMEM(w_gate.shape, BF16)] * 3),
        in_specs=[anywhere] * 5,
        out_specs=(pl.BlockSpec(memory_space=pltpu.VMEM),) * 4,
        scratch_shapes=[
            pltpu.VMEM((2, depth, length), BF16),
            pltpu.VMEM((2, 4, 2, length, depth), BF16),
            pltpu.VMEM((2, depth, 8 * length), BF16),
            pltpu.VMEM((chunks, depth, 3 * CHUNK), BF16),
            *[pltpu.VMEM((chunks, 4, 2, length, w), BF16) for w in wide],
            *[pltpu.VMEM((chunks, 7, length, w), BF16) for w in wide],
            *[pltpu.VMEM((chunks, 4, 2, length, w), BF16) for w in wide],
            pltpu.VMEM((4, 2, length, depth), F32),
            pltpu.VMEM((8, length, depth), BF16),
            pltpu.VMEM((length, depth), BF16),
            dma((2,)),
            dma((chunks, 2)),
            dma((2, 4)),
            dma((2,)),
            dma((2, chunks, 6)),
            dma((2, 2, chunks)),
            dma(()),
            dma(()),
            dma(()),
            dma(()),
        ],
        compiler_params=pltpu.CompilerParams(
            collective_id=0, has_side_effects=True, vmem_limit_bytes=58_800_000
        ),
        name="geglu_relay",
    )(jnp.swapaxes(normed, 1, 2), jnp.swapaxes(cotangent, 1, 2), w_gate, w_up, w_down)
    return (jnp.swapaxes(passed, 1, 2), *grads)


def solution(mesh):
    in_specs = (
        P("section", "tp", "fsdp"),
        P("section", "tp", "fsdp"),
        P("section", "fsdp", "tp"),
        P("section", "fsdp", "tp"),
        P("section", "fsdp", "tp"),
    )
    out_specs = (
        P("section", "tp", "fsdp"),
        P("section", "fsdp", "tp"),
        P("section", "fsdp", "tp"),
        P("section", "fsdp", "tp"),
    )
    return jax.shard_map(local, mesh=mesh, in_specs=in_specs, out_specs=out_specs, check_vma=False)
```
